256 devices in a mesh: parts: 2 (over y), gz: 32 (over z, core), shot: 4 (over x).
Axes of the slice: x: 4, y: 2, z: 16, core: 2. Of those that a mesh axis runs over, the one named last changes fastest.
The devices are a block of a 4x16x16 slice.
Arguments:
- wavefields: float32 [8, 2, 9, 128, 32, 128], P(('parts', 'shot'), None, None, 'gz'), parts along dimension 0, may hold values from -6 to 6
- earth_model: float32 [6, 128, 32, 128], P('parts', 'gz'), parts along dimension 0, may hold values from 0.4 to 1.6
- source_depth: int32 [8], P(('parts', 'shot')), parts along dimension 0, may hold values from 0 to 127
- source_column: int32 [8], P(('parts', 'shot')), parts along dimension 0, may hold values from 0 to 4095
- wavelet: float32 [8, 8], P(('parts', 'shot')), parts along dimension 0, may hold values from -30 to 30
- receiver_depth: int32 [8, 64], P(('parts', 'shot')), parts along dimension 0, may hold values from 0 to 127
- receiver_column: int32 [8, 64], P(('parts', 'shot')), parts along dimension 0, may hold values from 0 to 4095
- traces: float32 [8, 8, 64], P(('parts', 'shot')), parts along dimension 0, may hold values from -30 to 30
Outputs:
- images: float32 [4, 128, 32, 128], P('parts', 'gz'), parts along dimension 0
The draws below stay inside these ranges and needn't reach their ends.
There are 2 independent parts, one for each index of `parts`. The reference program is written for one: setup_inputs(seed, part) draws one part's arguments, and reference() takes and returns one part's arrays. A program takes and returns all parts, laid end to end along the dimension named above; each array names one. Nothing has to cross between parts.
All inputs are finite; a program needn't handle non-finite values.
Results may differ from the reference program's by a relative error of at most 0.00002.
Values sent between devices are 32-bit elements; how exact they have to be, the bound alone decides.
A program may use at most 64 MiB of HBM per device.

```python
import math
import jax
import jax.numpy as jnp
from jax import lax

NX = 32
NY = 128
STEPS = 8
RECV = 64
NZ = 128
SHOTS = 4


def plant(drawn, key, smallest, top_value):
    dims = drawn.shape
    spot = [jax.random.randint(jax.random.fold_in(key, axis), (), 0, dims[axis]) for axis in range(len(dims))]
    drawn = drawn.at[tuple(spot)].set(smallest)
    longest = dims.index(max(dims))
    spot[longest] = (spot[longest] + 1) % dims[longest]
    return drawn.at[tuple(spot)].set(top_value)


def levels(stream_key, extent, pieces, least, top_value):
    loudness = 1.0
    for position, parts in pieces:
        heights = jax.random.uniform(jax.random.fold_in(jax.random.fold_in(stream_key, 6), position), (parts,), jnp.float32, least / len(pieces), top_value / len(pieces))
        loudness = loudness * jnp.repeat(jnp.exp(heights), extent[position] // parts).reshape((-1,) + (1,) * (len(extent) - 1 - position))
    return loudness


def noise(stream_key, shape, scale, most, cuts=(), held_as=jnp.bfloat16):
    result = scale * jax.random.normal(stream_key, shape, jnp.float32)
    if cuts:
        result = result * levels(stream_key, shape, cuts, -0.22, 0.18)
    return jnp.clip(result, -most, most).astype(held_as)


def setup_inputs(seed: int = 0, part: int = 0) -> dict:
    key_list = jax.random.split(jax.random.key(seed), 9)
    part_keys = jax.random.split(jax.random.fold_in(key_list[8], part), 9)
    return {
        "wavefields": noise(part_keys[0], (SHOTS, 2, 9, NZ, NX, NY), 1.0, 6.0, ((0, 4), (3, 32)), jnp.float32),
        "earth_model": jnp.clip(jnp.exp(math.log(1.6) - 1.3862944 * jax.random.uniform(part_keys[1], (3, NZ, NX, NY), jnp.float32) ** levels(part_keys[1], (3, NZ, NX, NY), ((1, 32),), -0.2, 0.2)), 0.4, 1.6),
        "source_depth": plant(jax.random.randint(part_keys[2], (SHOTS,), 0, NZ), jax.random.fold_in(part_keys[2], 1), 0, NZ - 1).astype(jnp.int32),
        "source_column": plant(jax.random.randint(part_keys[3], (SHOTS,), 0, NX * NY), jax.random.fold_in(part_keys[3], 1), 0, (NX * NY) - 1).astype(jnp.int32),
        "wavelet": noise(part_keys[4], (SHOTS, STEPS), 5.0, 30.0, ((0, 4),), jnp.float32),
        "receiver_depth": plant(jax.random.randint(part_keys[5], (SHOTS, RECV), 0, NZ), jax.random.fold_in(part_keys[5], 1), 0, NZ - 1).astype(jnp.int32),
        "receiver_column": plant(jax.random.randint(part_keys[6], (SHOTS, RECV), 0, NX * NY), jax.random.fold_in(part_keys[6], 1), 0, (NX * NY) - 1).astype(jnp.int32),
        "traces": noise(part_keys[7], (SHOTS, STEPS, RECV), 5.0, 30.0, ((0, 4),), jnp.float32),
    }


time_step = 0.15


def forward_diff(array, dim_index):
    length = array.shape[dim_index]
    following = jnp.concatenate([lax.slice_in_dim(array, 1, length, axis=dim_index), jnp.zeros_like(lax.slice_in_dim(array, 0, 1, axis=dim_index))], axis=dim_index)
    return following - array


def backward_diff(array, dim_index):
    length = array.shape[dim_index]
    previous = jnp.concatenate([jnp.zeros_like(lax.slice_in_dim(array, 0, 1, axis=dim_index)), lax.slice_in_dim(array, 0, length - 1, axis=dim_index)], axis=dim_index)
    return array - previous


def depth_forward(array, plane_high):
    following = jnp.concatenate([array[:, 1:], plane_high[:, None]], axis=1)
    return following - array


def depth_backward(array, plane_low):
    previous = jnp.concatenate([plane_low[:, None], array[:, :-1]], axis=1)
    return array - previous


def velocity_half(fields, buoyancy, sxz_low, syz_low, szz_high):
    vel_x, vel_y, vel_z, sig_xx, sig_yy, sig_zz, sig_xy, sig_xz, sig_yz = fields
    vel_x = vel_x + time_step * buoyancy * (forward_diff(sig_xx, 2) + backward_diff(sig_xy, 3) + depth_backward(sig_xz, sxz_low))
    vel_y = vel_y + time_step * buoyancy * (backward_diff(sig_xy, 2) + forward_diff(sig_yy, 3) + depth_backward(sig_yz, syz_low))
    vel_z = vel_z + time_step * buoyancy * (backward_diff(sig_xz, 2) + backward_diff(sig_yz, 3) + depth_forward(sig_zz, szz_high))
    return vel_x, vel_y, vel_z


def stress_half(fields, lame_lambda, shear_mu, vz_low, vx_high, vy_high):
    vel_x, vel_y, vel_z, sig_xx, sig_yy, sig_zz, sig_xy, sig_xz, sig_yz = fields
    strain_x = backward_diff(vel_x, 2)
    strain_y = backward_diff(vel_y, 3)
    strain_z = depth_backward(vel_z, vz_low)
    spread = strain_x + strain_y + strain_z
    sig_xx = sig_xx + time_step * (lame_lambda * spread + 2.0 * shear_mu * strain_x)
    sig_yy = sig_yy + time_step * (lame_lambda * spread + 2.0 * shear_mu * strain_y)
    sig_zz = sig_zz + time_step * (lame_lambda * spread + 2.0 * shear_mu * strain_z)
    vx_up = depth_forward(vel_x, vx_high)
    vy_up = depth_forward(vel_y, vy_high)
    vz_along_x = forward_diff(vel_z, 2)
    vz_along_y = forward_diff(vel_z, 3)
    vx_along_y = forward_diff(vel_x, 3)
    vy_along_x = forward_diff(vel_y, 2)
    sig_xy = sig_xy + time_step * shear_mu * (vx_along_y + vy_along_x)
    sig_xz = sig_xz + time_step * shear_mu * (vx_up + vz_along_x)
    sig_yz = sig_yz + time_step * shear_mu * (vy_up + vz_along_y)
    rotation = (vz_along_y - vy_up) + (vx_up - vz_along_x) + (vy_along_x - vx_along_y)
    return [vel_x, vel_y, vel_z, sig_xx, sig_yy, sig_zz, sig_xy, sig_xz, sig_yz], rotation


def reference(wavefields, earth_model, source_depth, source_column, wavelet, receiver_depth, receiver_column, traces):
    buoyancy = earth_model[0]
    lame_lambda = earth_model[1]
    shear_mu = earth_model[2]
    image_pp = jnp.zeros((NZ, NX, NY), jnp.float32)
    image_ps = jnp.zeros((NZ, NX, NY), jnp.float32)
    zero_plane = jnp.zeros((2, NX, NY), jnp.float32)
    for shot_index in range(SHOTS):
        fields = [wavefields[shot_index, :, field_no] for field_no in range(9)]
        src_row = source_column[shot_index] // NY
        src_col = source_column[shot_index] % NY
        rec_row = receiver_column[shot_index] // NY
        rec_col = receiver_column[shot_index] % NY
        for step_index in range(STEPS):
            vel_x, vel_y, vel_z = velocity_half(fields, buoyancy, zero_plane, zero_plane, zero_plane)
            vel_z = vel_z.at[1, receiver_depth[shot_index], rec_row, rec_col].add(time_step * traces[shot_index, step_index])
            fields, rotation = stress_half([vel_x, vel_y, vel_z] + list(fields[3:]), lame_lambda, shear_mu, zero_plane, zero_plane, zero_plane)
            for field_no in (3, 4, 5):
                fields[field_no] = fields[field_no].at[0, source_depth[shot_index], src_row, src_col].add(time_step * wavelet[shot_index, step_index])
            pressure = (fields[3] + fields[4] + fields[5]) / 3.0
            image_pp = image_pp + pressure[0] * pressure[1]
            image_ps = image_ps + pressure[0] * rotation[1]
    return jnp.stack([image_pp, image_ps]) / STEPS
```

```python
import functools

import jax
import jax.numpy as jnp
from jax import lax
from jax.experimental import pallas as pl
from jax.experimental.pallas import tpu as pltpu
from jax.sharding import PartitionSpec as P

MESH = pl.DeviceIdType.MESH
time_step = 0.15
GUARD = 8
SXX, SYY, SZZ, SXY, SXZ, SYZ = range(6)


def window_kernel(
    dims,
    fields_in,
    earth_in,
    source_depth,
    source_column,
    wavelet,
    receiver_depth,
    receiver_column,
    traces,
    out,
    vel,
    vel_halo,
    sig,
    sig_halo,
    mat,
    mat_halo,
    source_at,
    inject,
    press,
    image,
    partial,
    landed,
    load_sem,
    first_send,
    first_recv,
    step_send,
    step_recv,
    sum_send,
    sum_recv,
):
    slabs, shots, depth, rows, cols, steps, receivers = dims
    here = lax.axis_index("gz")
    shot = lax.axis_index("shot")
    top, bottom = here > 0, here < slabs - 1
    last = depth - 1
    body = pl.ds(GUARD, rows)
    after = pl.ds(GUARD + 1, rows)
    before = pl.ds(GUARD - 1, rows)
    lane = lax.broadcasted_iota(jnp.int32, (rows, cols), 1)
    row = lax.broadcasted_iota(jnp.int32, (rows, cols), 0)
    at_first, at_last = lane == 0, lane == cols - 1
    partners = (shot + 1 - 2 * lax.rem(shot, 2), shots - 1 - shot)

    def b_y(f):
        return f - jnp.where(at_first, 0.0, pltpu.roll(f, 1, 1))

    def f_y(f):
        return jnp.where(at_last, 0.0, pltpu.roll(f, cols - 1, 1)) - f

    loads = [
        pltpu.make_async_copy(
            fields_in.at[:, 3:9], sig.at[:, :, :, body, :], load_sem.at[0]
        ),
        pltpu.make_async_copy(
            fields_in.at[:, 0:3], vel.at[:, :, :, body, :], load_sem.at[1]
        ),
        pltpu.make_async_copy(earth_in, mat, load_sem.at[2]),
    ]
    for copy in loads:
        copy.start()

    vel_halo[...] = jnp.zeros_like(vel_halo)
    sig_halo[...] = jnp.zeros_like(sig_halo)
    mat_halo[...] = jnp.zeros_like(mat_halo)

    barrier = pltpu.get_barrier_semaphore()

    @pl.when(top)
    def _():
        pl.semaphore_signal(barrier, inc=1, device_id={"gz": here - 1}, device_id_type=MESH)

    @pl.when(bottom)
    def _():
        pl.semaphore_signal(barrier, inc=1, device_id={"gz": here + 1}, device_id_type=MESH)

    for partner in partners:
        pl.semaphore_signal(barrier, inc=1, device_id={"shot": partner}, device_id_type=MESH)

    edge = pl.ds(0, GUARD)
    tail = pl.ds(GUARD + rows, GUARD)
    zeros = jnp.zeros((GUARD, cols), jnp.float32)
    for ref, count in ((vel, 3), (sig, 6)):
        for w in range(2):
            for c in range(count):
                for z in range(depth):
                    ref[w, c, z, edge, :] = zeros
                    ref[w, c, z, tail, :] = zeros

    have_top = jnp.where(top, 1, 0)
    have_bottom = jnp.where(bottom, 1, 0)
    pl.semaphore_wait(barrier, 2 + have_top + have_bottom)

    def remote(src, dst, send, recv, **to):
        return pltpu.make_async_remote_copy(
            src_ref=src, dst_ref=dst, send_sem=send, recv_sem=recv, device_id=to, device_id_type=MESH
        )

    first_down = [
        remote(fields_in.at[:, 7:9, last], sig_halo.at[:, 0:2], first_send.at[0], first_recv.at[0], gz=here + 1),
        remote(earth_in.at[2, last], mat_halo.at[0], first_send.at[1], first_recv.at[1], gz=here + 1),
    ]
    first_up = [
        remote(fields_in.at[:, 5, 0], sig_halo.at[:, 2], first_send.at[2], first_recv.at[2], gz=here - 1),
        remote(earth_in.at[1:3, 0], mat_halo.at[1:3], first_send.at[3], first_recv.at[3], gz=here - 1),
    ]

    @pl.when(bottom)
    def _():
        for copy in first_down:
            copy.start()

    @pl.when(top)
    def _():
        for copy in first_up:
            copy.start()

    def velocity_copies(w, slot):
        down = remote(
            vel.at[w, :, last, body, :],
            vel_halo.at[slot, 0, w, :, body, :],
            step_send.at[slot, 0, w],
            step_recv.at[slot, 0, w],
            gz=here + 1,
        )
        up = remote(
            vel.at[w, :, 0, body, :],
            vel_halo.at[slot, 1, w, :, body, :],
            step_send.at[slot, 1, w],
            step_recv.at[slot, 1, w],
            gz=here - 1,
        )
        return down, up

    def send_velocity(w, slot):
        down, up = velocity_copies(w, slot)

        @pl.when(bottom)
        def _():
            down.start()

        @pl.when(top)
        def _():
            up.start()

    def velocity_arrived(w, slot):
        down, up = velocity_copies(w, slot)

        @pl.when(top)
        def _():
            down.wait_recv()

        @pl.when(bottom)
        def _():
            up.wait_recv()

    def velocity_left(w, slot):
        down, up = velocity_copies(w, slot)

        @pl.when(bottom)
        def _():
            down.wait_send()

        @pl.when(top)
        def _():
            up.wait_send()

    source_row = (source_depth[0] - here * depth) * rows + source_column[0] // cols
    source_col = source_column[0] % cols
    for z in range(depth + 1):
        hit = (row + z * rows == source_row) & (lane == source_col)
        source_at[z] = jnp.where(hit, time_step, 0.0)
    cells = depth * rows
    receiver_row = (receiver_depth[...] - here * depth) * rows + receiver_column[...] // cols
    receiver_col = receiver_column[...] % cols
    in_row = lax.broadcasted_iota(jnp.int32, (cells, receivers), 0) == receiver_row
    in_col = lax.broadcasted_iota(jnp.int32, (cols, receivers), 0) == receiver_col
    in_col = jnp.where(in_col, 1.0, 0.0)
    for n in range(steps):
        amount = jnp.where(in_row, time_step * traces[0, pl.ds(n, 1), :], 0.0)
        inject[n] = lax.dot_general(
            amount,
            in_col,
            (((1,), (1,)), ((), ())),
            precision=lax.Precision.HIGHEST,
            preferred_element_type=jnp.float32,
        ).reshape(depth, rows, cols)
    image[...] = jnp.zeros_like(image)

    for copy in loads:
        copy.wait()
    mat[...] = time_step * mat[...]

    @pl.when(top)
    def _():
        for copy in first_down:
            copy.wait_recv()

    @pl.when(bottom)
    def _():
        for copy in first_up:
            copy.wait_recv()

    mat_halo[...] = time_step * mat_halo[...]

    def update_velocity(w, z, n):
        buoyancy = mat[0, z]
        sxx, syy, szz, sxy, sxz, syz = [sig[w, c, z, body, :] for c in range(6)]
        sxz_low = sig_halo[w, 0] if z == 0 else sig[w, SXZ, z - 1, body, :]
        syz_low = sig_halo[w, 1] if z == 0 else sig[w, SYZ, z - 1, body, :]
        szz_high = sig_halo[w, 2] if z == last else sig[w, SZZ, z + 1, body, :]
        fx = (sig[w, SXX, z, after, :] - sxx) + b_y(sxy) + (sxz - sxz_low)
        fy = (sxy - sig[w, SXY, z, before, :]) + f_y(syy) + (syz - syz_low)
        fz = (sxz - sig[w, SXZ, z, before, :]) + b_y(syz) + (szz_high - szz)
        vel[w, 0, z, body, :] = vel[w, 0, z, body, :] + buoyancy * fx
        vel[w, 1, z, body, :] = vel[w, 1, z, body, :] + buoyancy * fy
        moved = vel[w, 2, z, body, :] + buoyancy * fz
        if w == 1:
            moved = moved + inject[n, z]
        vel[w, 2, z, body, :] = moved

    def update_normal(w, z, n, slot):
        vx, vy, vz = [vel[w, c, z, body, :] for c in range(3)]
        vz_low = vel_halo[slot, 0, w, 2, body, :] if z == 0 else vel[w, 2, z - 1, body, :]
        ex = vx - vel[w, 0, z, before, :]
        ey = b_y(vy)
        ez = vz - vz_low
        common = mat[1, z] * (ex + ey + ez)
        twice = 2.0 * mat[2, z]
        if w == 0:
            common = common + source_at[z] * wavelet[0, n]
        sxx = sig[w, SXX, z, body, :] + (common + twice * ex)
        syy = sig[w, SYY, z, body, :] + (common + twice * ey)
        szz = sig[w, SZZ, z, body, :] + (common + twice * ez)
        sig[w, SXX, z, body, :] = sxx
        sig[w, SYY, z, body, :] = syy
        sig[w, SZZ, z, body, :] = szz
        pressure = (sxx + syy + szz) * (1.0 / 3.0)
        if w == 0:
            press[z] = pressure
        else:
            image[0, z] = image[0, z] + press[z] * pressure

    def update_shear(w, z, slot):
        vx, vy, vz = [vel[w, c, z, body, :] for c in range(3)]
        vx_high = vel_halo[slot, 1, w, 0, body, :] if z == last else vel[w, 0, z + 1, body, :]
        vy_high = vel_halo[slot, 1, w, 1, body, :] if z == last else vel[w, 1, z + 1, body, :]
        x_up = vx_high - vx
        y_up = vy_high - vy
        z_along_x = vel[w, 2, z, after, :] - vz
        z_along_y = f_y(vz)
        x_along_y = f_y(vx)
        y_along_x = vel[w, 1, z, after, :] - vy
        mu = mat[2, z]
        sig[w, SXY, z, body, :] = sig[w, SXY, z, body, :] + mu * (x_along_y + y_along_x)
        sig[w, SXZ, z, body, :] = sig[w, SXZ, z, body, :] + mu * (x_up + z_along_x)
        sig[w, SYZ, z, body, :] = sig[w, SYZ, z, body, :] + mu * (y_up + z_along_y)
        if w == 1:
            rotation = (z_along_y - y_up) + (x_up - z_along_x) + (y_along_x - x_along_y)
            image[1, z] = image[1, z] + press[z] * rotation

    def update_halo(w, n, slot):
        vx, vy, vz = [vel_halo[slot, 0, w, c, body, :] for c in range(3)]
        mu = mat_halo[0]
        x_term = (vel[w, 0, 0, body, :] - vx) + (vel_halo[slot, 0, w, 2, after, :] - vz)
        y_term = (vel[w, 1, 0, body, :] - vy) + f_y(vz)
        sig_halo[w, 0] = sig_halo[w, 0] + mu * x_term
        sig_halo[w, 1] = sig_halo[w, 1] + mu * y_term
        vx, vy, vz = [vel_halo[slot, 1, w, c, body, :] for c in range(3)]
        ex = vx - vel_halo[slot, 1, w, 0, before, :]
        ez = vz - vel[w, 2, last, body, :]
        change = mat_halo[1] * (ex + b_y(vy) + ez) + 2.0 * mat_halo[2] * ez
        if w == 0:
            change = change + source_at[depth] * wavelet[0, n]
        sig_halo[w, 2] = sig_halo[w, 2] + change

    inner = range(1, last)

    def stress_inside(n, slot):
        for w in range(2):
            for z in range(1, depth):
                update_normal(w, z, n, slot)
            if w == 0:
                for z in range(last):
                    update_shear(w, z, slot)
            else:
                for z in range(1, last):
                    update_shear(w, z, slot)

    def stress_edge(w, n, slot):
        update_normal(w, 0, n, slot)
        if w == 1:
            update_shear(w, 0, slot)
        update_shear(w, last, slot)

    for w in range(2):
        update_velocity(w, 0, 0)
        update_velocity(w, last, 0)
        send_velocity(w, 0)
    for w in range(2):
        for z in inner:
            update_velocity(w, z, 0)

    def step(n, carry):
        slot = lax.rem(n, 2)
        stress_inside(n, slot)
        for w in range(2):
            velocity_arrived(w, slot)
            stress_edge(w, n, slot)
            update_halo(w, n, slot)
            velocity_left(w, slot)
            update_velocity(w, 0, n + 1)
            update_velocity(w, last, n + 1)
            send_velocity(w, 1 - slot)
        for w in range(2):
            for z in inner:
                update_velocity(w, z, n + 1)
        return carry

    lax.fori_loop(0, steps - 1, step, 0)

    end = steps - 1
    slot = end % 2
    stress_inside(end, slot)
    for w in range(2):
        velocity_arrived(w, slot)
        stress_edge(w, end, slot)
        velocity_left(w, slot)

    first_round = [
        remote(image.at[i], landed.at[0, i], sum_send.at[0, i], sum_recv.at[0, i], shot=partners[i])
        for i in range(2)
    ]
    second_round = [
        remote(partial.at[i], landed.at[1, i], sum_send.at[1, i], sum_recv.at[1, i], shot=partners[1 - i])
        for i in range(2)
    ]
    for i in range(2):
        first_round[i].start()
    for i in range(2):
        first_round[i].wait_recv()
        partial[i] = image[i] + landed[0, i]
        second_round[i].start()
    for i in range(2):
        second_round[i].wait_recv()
        out[i] = partial[i] + landed[1, i]
    for i in range(2):
        first_round[i].wait_send()
        second_round[i].wait_send()

    @pl.when(bottom)
    def _():
        for copy in first_down:
            copy.wait_send()

    @pl.when(top)
    def _():
        for copy in first_up:
            copy.wait_send()


def solution(mesh):
    slabs, shots = mesh.shape["gz"], mesh.shape["shot"]

    def on_device(wavefields, earth, s_depth, s_column, wavelet, r_depth, r_column, traces):
        depth, rows, cols = earth.shape[1:]
        steps, receivers = traces.shape[1:]
        dims = (slabs, shots, depth, rows, cols, steps, receivers)
        padded = rows + 2 * GUARD
        f32 = jnp.float32
        any_spec = pl.BlockSpec(memory_space=pl.ANY)
        smem = pl.BlockSpec(memory_space=pltpu.SMEM)
        vmem = pl.BlockSpec(memory_space=pltpu.VMEM)
        dma = pltpu.SemaphoreType.DMA
        summed = pl.pallas_call(
            functools.partial(window_kernel, dims),
            out_shape=jax.ShapeDtypeStruct((2, depth, rows, cols), f32),
            in_specs=[any_spec, any_spec, smem, smem, smem, vmem, vmem, vmem],
            out_specs=vmem,
            scratch_shapes=[
                pltpu.VMEM((2, 3, depth, padded, cols), f32),
                pltpu.VMEM((2, 2, 2, 3, padded, cols), f32),
                pltpu.VMEM((2, 6, depth, padded, cols), f32),
                pltpu.VMEM((2, 3, rows, cols), f32),
                pltpu.VMEM((3, depth, rows, cols), f32),
                pltpu.VMEM((3, rows, cols), f32),
                pltpu.VMEM((depth + 1, rows, cols), f32),
                pltpu.VMEM((steps, depth, rows, cols), f32),
                pltpu.VMEM((depth, rows, cols), f32),
                pltpu.VMEM((2, depth, rows, cols), f32),
                pltpu.VMEM((2, depth, rows, cols), f32),
                pltpu.VMEM((2, 2, depth, rows, cols), f32),
                dma((3,)),
                dma((4,)),
                dma((4,)),
                dma((2, 2, 2)),
                dma((2, 2, 2)),
                dma((2, 2)),
                dma((2, 2)),
            ],
            compiler_params=pltpu.CompilerParams(collective_id=0, has_side_effects=True),
        )(wavefields[0], earth, s_depth, s_column, wavelet, r_depth, r_column, traces)
        return summed / steps

    sharded = P(("parts", "shot"))
    return jax.shard_map(
        on_device,
        mesh=mesh,
        in_specs=(
            P(("parts", "shot"), None, None, "gz", None, None),
            P("parts", "gz", None, None),
            sharded,
            sharded,
            P(("parts", "shot"), None),
            P(("parts", "shot"), None),
            P(("parts", "shot"), None),
            P(("parts", "shot"), None, None),
        ),
        out_specs=P("parts", "gz", None, None),
        check_vma=False,
    )
```

```python
import functools

import jax
import jax.numpy as jnp
from jax import lax
from jax.experimental import pallas as pl
from jax.experimental.pallas import tpu as pltpu
from jax.sharding import PartitionSpec as P

MESH = pl.DeviceIdType.MESH
time_step = 0.15
GUARD = 8
SXX, SYY, SZZ, SXY, SXZ, SYZ = range(6)


def window_kernel(
    dims,
    fields_in,
    earth_in,
    source_depth_in,
    source_column_in,
    wavelet_in,
    receiver_depth_in,
    receiver_column_in,
    traces_in,
    out,
    vel,
    vel_msg,
    vel_mid,
    vel_near,
    sig,
    sig_near,
    sig_far,
    mat,
    mat_near,
    mat_far,
    source_at,
    inject,
    press,
    spin,
    image,
    partial,
    landed,
    source_depth,
    source_column,
    wavelet,
    receiver_depth,
    receiver_column,
    traces,
    load_sem,
    small_sem,
    first_send,
    first_recv,
    msg_send,
    msg_recv,
    mid_send,
    mid_recv,
    sum_send,
    sum_recv,
):
    slabs, shots, depth, rows, cols, steps, receivers = dims
    here = lax.axis_index("gz")
    shot = lax.axis_index("shot")
    has_up, has_down = here > 0, here < slabs - 1
    last = depth - 1
    whole = pl.ds(0, rows)
    body = pl.ds(GUARD, rows)
    after = pl.ds(GUARD + 1, rows)
    before = pl.ds(GUARD - 1, rows)
    lane = lax.broadcasted_iota(jnp.int32, (rows, cols), 1)
    row = lax.broadcasted_iota(jnp.int32, (rows, cols), 0)
    at_first, at_last = lane == 0, lane == cols - 1
    partners = (shot + 1 - 2 * lax.rem(shot, 2), shots - 1 - shot)

    def b_y(f):
        return f - jnp.where(at_first, 0.0, pltpu.roll(f, 1, 1))

    def f_y(f):
        return jnp.where(at_last, 0.0, pltpu.roll(f, cols - 1, 1)) - f

    loads = [
        pltpu.make_async_copy(
            fields_in.at[:, 3:9], sig.at[:, :, :, body, :], load_sem.at[0]
        ),
        pltpu.make_async_copy(
            fields_in.at[:, 0:3], vel.at[1, :, :, :, body, :], load_sem.at[1]
        ),
        pltpu.make_async_copy(earth_in, mat, load_sem.at[2]),
    ]
    small = [
        pltpu.make_async_copy(src, dst, small_sem.at[i])
        for i, (src, dst) in enumerate(
            (
                (source_depth_in, source_depth),
                (source_column_in, source_column),
                (wavelet_in, wavelet),
                (receiver_depth_in, receiver_depth),
                (receiver_column_in, receiver_column),
                (traces_in, traces),
            )
        )
    ]
    for copy in loads + small:
        copy.start()

    for ref in (vel_msg, vel_mid, sig_near, sig_far, mat_near, mat_far):
        ref[...] = jnp.zeros_like(ref)

    barrier = pltpu.get_barrier_semaphore()

    def up_to(where, then):
        @pl.when(where)
        def _():
            then()

    def greet(**to):
        pl.semaphore_signal(barrier, inc=1, device_id=to, device_id_type=MESH)

    up_to(has_down, lambda: greet(gz=here + 1))
    up_to(has_up, lambda: greet(gz=here - 1))
    for partner in partners:
        greet(shot=partner)

    edge = pl.ds(0, GUARD)
    tail = pl.ds(GUARD + rows, GUARD)
    zeros = jnp.zeros((GUARD, cols), jnp.float32)
    for w in range(2):
        for z in range(depth):
            for c in range(6):
                sig[w, c, z, edge, :] = zeros
                sig[w, c, z, tail, :] = zeros
            for c in range(3):
                for parity in range(2):
                    vel[parity, w, c, z, edge, :] = zeros
                    vel[parity, w, c, z, tail, :] = zeros
        for c in range(3):
            for side in range(2):
                vel_near[side, w, c, edge, :] = zeros
                vel_near[side, w, c, tail, :] = zeros

    pl.semaphore_wait(barrier, 2 + jnp.where(has_up, 1, 0) + jnp.where(has_down, 1, 0))

    def remote(src, dst, send, recv, **to):
        return pltpu.make_async_remote_copy(
            src_ref=src, dst_ref=dst, send_sem=send, recv_sem=recv, device_id=to, device_id_type=MESH
        )

    downs = (
        (fields_in.at[:, 7:9, last], sig_near.at[0, :, 4:6, body, :]),
        (fields_in.at[:, 3:7, last], sig_near.at[0, :, 0:4, body, :]),
        (fields_in.at[:, 7:9, last - 1], sig_far.at[:, 0:2]),
        (earth_in.at[:, last], mat_near.at[0]),
        (earth_in.at[2, last - 1], mat_far.at[0]),
    )
    ups = (
        (fields_in.at[:, 5:6, 0], sig_near.at[1, :, 2:3, body, :]),
        (fields_in.at[:, 3:5, 0], sig_near.at[1, :, 0:2, body, :]),
        (fields_in.at[:, 6:9, 0], sig_near.at[1, :, 3:6, body, :]),
        (fields_in.at[:, 5, 1], sig_far.at[:, 2]),
        (earth_in.at[:, 0], mat_near.at[1]),
        (earth_in.at[1:3, 1], mat_far.at[1:3]),
    )
    first_down = [
        remote(src, dst, first_send.at[0, i], first_recv.at[0, i], gz=here + 1)
        for i, (src, dst) in enumerate(downs)
    ]
    first_up = [
        remote(src, dst, first_send.at[1, i], first_recv.at[1, i], gz=here - 1)
        for i, (src, dst) in enumerate(ups)
    ]
    up_to(has_down, lambda: [copy.start() for copy in first_down])
    up_to(has_up, lambda: [copy.start() for copy in first_up])

    def message(w, slot, side):
        planes = pl.ds(depth - 2, 2) if side == 0 else pl.ds(0, 2)
        return remote(
            vel.at[0, w, :, planes, body, :],
            vel_msg.at[slot, side, w, :, :, body, :],
            msg_send.at[slot, side, w],
            msg_recv.at[slot, side, w],
            gz=here + 1 if side == 0 else here - 1,
        )

    def middle(w, cycle, side):
        return remote(
            vel.at[1, w, :, depth - 2 if side == 0 else 1, body, :],
            vel_mid.at[cycle, side, w, :, body, :],
            mid_send.at[cycle, side, w],
            mid_recv.at[cycle, side, w],
            gz=here + 1 if side == 0 else here - 1,
        )

    goes = (has_down, has_up)
    comes = (has_up, has_down)

    for copy in small:
        copy.wait()
    source_row = (source_depth[0] - here * depth + 1) * rows + source_column[0] // cols
    source_col = source_column[0] % cols
    for z in range(depth + 3):
        hit = (row + z * rows == source_row) & (lane == source_col)
        source_at[z] = jnp.where(hit, time_step, 0.0)
    cells = (depth + 2) * rows
    receiver_row = (receiver_depth[...] - here * depth + 1) * rows + receiver_column[...] // cols
    receiver_col = receiver_column[...] % cols
    in_row = lax.broadcasted_iota(jnp.int32, (cells, receivers), 0) == receiver_row
    in_col = lax.broadcasted_iota(jnp.int32, (cols, receivers), 0) == receiver_col
    in_col = jnp.where(in_col, 1.0, 0.0)

    def receivers_at(n, carry):
        amount = jnp.where(in_row, time_step * traces[0, pl.ds(n, 1), :], 0.0)
        inject[n] = lax.dot_general(
            amount,
            in_col,
            (((1,), (1,)), ((), ())),
            precision=lax.Precision.HIGHEST,
            preferred_element_type=jnp.float32,
        ).reshape(depth + 2, rows, cols)
        return carry

    lax.fori_loop(0, steps, receivers_at, 0)
    image[...] = jnp.zeros_like(image)

    for copy in loads:
        copy.wait()
    mat[...] = time_step * mat[...]

    def v(parity, slot, w, c, e, at=body):
        if 0 <= e < depth:
            return vel[parity, w, c, e, at, :]
        side = 0 if e < 0 else 1
        if parity == 0:
            return vel_msg[slot, side, w, c, e + 2 if e < 0 else e - depth, at, :]
        if e in (-1, depth):
            return vel_near[side, w, c, at, :]
        return vel_mid[slot, side, w, c, at, :]

    def s_at(w, f, e):
        if 0 <= e < depth:
            return sig, (w, f, e), True
        if e in (-1, depth):
            return sig_near, (0 if e < 0 else 1, w, f), True
        return sig_far, (w, {SXZ: 0, SYZ: 1, SZZ: 2}[f]), False

    def s(w, f, e, at=body):
        ref, index, guarded = s_at(w, f, e)
        return ref[(*index, at if guarded else whole, slice(None))]

    def add_s(w, f, e, change):
        ref, index, guarded = s_at(w, f, e)
        value = ref[(*index, body if guarded else whole, slice(None))] + change
        ref[(*index, body if guarded else whole, slice(None))] = value
        return value

    def m(which, e):
        if 0 <= e < depth:
            return mat[which, e]
        if e in (-1, depth):
            return mat_near[0 if e < 0 else 1, which]
        return mat_far[0 if e < 0 else which]

    def velocity(w, e, n, old, slot):
        sxx, syy, szz, sxy, sxz, syz = [s(w, f, e) for f in range(6)]
        fx = (s(w, SXX, e, after) - sxx) + b_y(sxy) + (sxz - s(w, SXZ, e - 1))
        fy = (sxy - s(w, SXY, e, before)) + f_y(syy) + (syz - s(w, SYZ, e - 1))
        fz = (sxz - s(w, SXZ, e, before)) + b_y(syz) + (s(w, SZZ, e + 1) - szz)
        buoyancy = m(0, e)
        moved = [v(old, slot, w, c, e) + buoyancy * f for c, f in enumerate((fx, fy, fz))]
        if w == 1:
            moved[2] = moved[2] + inject[n, e + 1]
        for c in range(3):
            if 0 <= e < depth:
                vel[1 - old, w, c, e, body, :] = moved[c]
            else:
                vel_near[0 if e < 0 else 1, w, c, body, :] = moved[c]

    def normal(parity, slot, w, e, n, spun=None):
        vx, vy, vz = [v(parity, slot, w, c, e) for c in range(3)]
        ex = vx - v(parity, slot, w, 0, e, before)
        ey = b_y(vy)
        ez = vz - v(parity, slot, w, 2, e - 1)
        common = m(1, e) * (ex + ey + ez)
        twice = 2.0 * m(2, e)
        if w == 0:
            common = common + source_at[e + 1] * wavelet[0, n]
        szz = add_s(w, SZZ, e, common + twice * ez)
        if e > depth:
            return
        sxx = add_s(w, SXX, e, common + twice * ex)
        syy = add_s(w, SYY, e, common + twice * ey)
        if not 0 <= e < depth:
            return
        pressure = (sxx + syy + szz) * (1.0 / 3.0)
        if w == 0:
            press[parity, e] = pressure
        else:
            image[0, e] = image[0, e] + press[parity, e] * pressure
            if spun is not None:
                image[1, e] = image[1, e] + press[parity, e] * spin[spun]

    def shear(parity, slot, w, e, spun=None):
        vx, vy, vz = [v(parity, slot, w, c, e) for c in range(3)]
        x_up = v(parity, slot, w, 0, e + 1) - vx
        y_up = v(parity, slot, w, 1, e + 1) - vy
        z_along_x = v(parity, slot, w, 2, e, after) - vz
        z_along_y = f_y(vz)
        x_along_y = f_y(vx)
        y_along_x = v(parity, slot, w, 1, e, after) - vy
        mu = m(2, e)
        add_s(w, SXY, e, mu * (x_along_y + y_along_x))
        add_s(w, SXZ, e, mu * (x_up + z_along_x))
        add_s(w, SYZ, e, mu * (y_up + z_along_y))
        if w == 1:
            rotation = (z_along_y - y_up) + (x_up - z_along_x) + (y_along_x - x_along_y)
            if spun is None:
                image[1, e] = image[1, e] + press[parity, e] * rotation
            else:
                spin[spun] = rotation

    def shear_flat(parity, slot, w, e):
        x_along_y = f_y(v(parity, slot, w, 0, e))
        y_along_x = v(parity, slot, w, 1, e, after) - v(parity, slot, w, 1, e)
        add_s(w, SXY, e, m(2, e) * (x_along_y + y_along_x))

    def shear_deep(parity, slot, w, e):
        vx, vy, vz = [v(parity, slot, w, c, e) for c in range(3)]
        mu = m(2, e)
        z_along_x = v(parity, slot, w, 2, e, after) - vz
        add_s(w, SXZ, e, mu * ((v(parity, slot, w, 0, e + 1) - vx) + z_along_x))
        add_s(w, SYZ, e, mu * ((v(parity, slot, w, 1, e + 1) - vy) + f_y(vz)))

    def inside(cycle, n, send):
        for w in range(2):
            for e in range(1, depth):
                normal(0, None, w, e, n)
            shear(0, None, w, 0, spun=0)
            for e in range(1, last):
                shear(0, None, w, e)
            for e in (1, 2):
                velocity(w, e, n + 1, 0, None)

            def start(w=w):
                for side in range(2):
                    up_to(goes[side], middle(w, cycle, side).start)

            if send is True:
                start()
            else:
                up_to(send, start)
            normal(1, None, w, 2, n + 1)
            shear(1, None, w, 1, spun=1)

    def lower(slot, w, n, final):
        up_to(comes[1], message(w, slot, 1).wait_recv)
        shear(0, slot, w, last)
        normal(0, slot, w, depth, n)
        shear_flat(0, slot, w, depth)
        shear_deep(0, slot, w, depth)
        normal(0, slot, w, depth + 1, n)
        velocity(w, last, n + 1, 0, slot)
        velocity(w, depth, n + 1, 0, slot)
        normal(1, slot, w, last, n + 1)
        shear(1, slot, w, last - 1)
        shear(1, slot, w, last)
        up_to(goes[0], message(w, slot, 0).wait_send)
        if final:
            return
        normal(1, slot, w, depth, n + 1)
        velocity(w, last, n + 2, 1, slot)
        velocity(w, last - 1, n + 2, 1, slot)
        up_to(goes[0], message(w, 1 - slot, 0).start)
        shear_flat(1, slot, w, depth)

    def upper(slot, w, n, final):
        up_to(comes[0], message(w, slot, 0).wait_recv)
        normal(0, slot, w, 0, n, spun=0)
        shear_deep(0, slot, w, -1)
        shear_flat(0, slot, w, -1)
        normal(0, slot, w, -1, n)
        shear_deep(0, slot, w, -2)
        velocity(w, 0, n + 1, 0, slot)
        velocity(w, -1, n + 1, 0, slot)
        normal(1, slot, w, 0, n + 1)
        normal(1, slot, w, 1, n + 1, spun=1)
        shear(1, slot, w, 0)
        up_to(goes[1], message(w, slot, 1).wait_send)
        if final:
            return
        shear_deep(1, slot, w, -1)
        velocity(w, 0, n + 2, 1, slot)
        velocity(w, 1, n + 2, 1, slot)
        up_to(goes[1], message(w, 1 - slot, 1).start)
        shear_flat(1, slot, w, -1)

    def catch_up(cycle, n):
        for w in range(2):
            up_to(comes[1], middle(w, cycle, 1).wait_recv)
            shear_deep(1, cycle, w, depth)
            normal(1, cycle, w, depth + 1, n)
            up_to(comes[0], middle(w, cycle, 0).wait_recv)
            normal(1, cycle, w, -1, n)
            shear_deep(1, cycle, w, -2)

    up_to(comes[1], first_up[0].wait_recv)
    for w in range(2):
        velocity(w, last, 0, 1, None)
        velocity(w, last - 1, 0, 1, None)
        up_to(goes[0], message(w, 0, 0).start)
    up_to(comes[0], first_down[0].wait_recv)
    for w in range(2):
        velocity(w, 0, 0, 1, None)
        velocity(w, 1, 0, 1, None)
        up_to(goes[1], message(w, 0, 1).start)
    inside(0, 0, True)
    up_to(comes[1], lambda: [copy.wait_recv() for copy in first_up[1:]])
    up_to(comes[0], lambda: [copy.wait_recv() for copy in first_down[1:]])
    mat_near[...] = time_step * mat_near[...]
    mat_far[...] = time_step * mat_far[...]

    cycles = steps // 2

    def cycle_body(cycle, carry):
        slot = lax.rem(cycle, 2)
        n = 2 * cycle
        for w in range(2):
            lower(slot, w, n, False)
        for w in range(2):
            upper(slot, w, n, False)
        for w in range(2):
            for side in range(2):
                up_to(goes[side], middle(w, cycle, side).wait_send)
        inside(cycle + 1, n + 2, cycle < cycles - 2)
        catch_up(cycle, n + 1)
        return carry

    lax.fori_loop(0, cycles - 1, cycle_body, 0)

    def first_round(half, i):
        planes = pl.ds(2 * half, 2)
        return remote(
            image.at[i, planes],
            landed.at[0, i, planes],
            sum_send.at[0, half, i],
            sum_recv.at[0, half, i],
            shot=partners[i],
        )

    def second_round(half, i):
        planes = pl.ds(2 * half, 2)
        return remote(
            partial.at[i, planes],
            landed.at[1, i, planes],
            sum_send.at[1, half, i],
            sum_recv.at[1, half, i],
            shot=partners[1 - i],
        )

    end = (cycles - 1) % 2
    for w in range(2):
        lower(end, w, steps - 2, True)
    for i in range(2):
        first_round(1, i).start()
    for w in range(2):
        upper(end, w, steps - 2, True)
    for i in range(2):
        first_round(0, i).start()
    for half in (1, 0):
        planes = pl.ds(2 * half, 2)
        for i in range(2):
            first_round(half, i).wait_recv()
            partial[i, planes] = image[i, planes] + landed[0, i, planes]
            second_round(half, i).start()
    for half in (1, 0):
        planes = pl.ds(2 * half, 2)
        for i in range(2):
            second_round(half, i).wait_recv()
            out[i, planes] = partial[i, planes] + landed[1, i, planes]
    for half in (1, 0):
        for i in range(2):
            first_round(half, i).wait_send()
            second_round(half, i).wait_send()
    up_to(has_down, lambda: [copy.wait_send() for copy in first_down])
    up_to(has_up, lambda: [copy.wait_send() for copy in first_up])


def solution(mesh):
    slabs, shots = mesh.shape["gz"], mesh.shape["shot"]

    def on_device(wavefields, earth, s_depth, s_column, wavelet, r_depth, r_column, traces):
        depth, rows, cols = earth.shape[1:]
        steps, receivers = traces.shape[1:]
        assert depth == 4 and shots == 4 and steps % 2 == 0 and steps >= 4
        dims = (slabs, shots, depth, rows, cols, steps, receivers)
        padded = rows + 2 * GUARD
        f32 = jnp.float32
        mids = steps // 2 - 1
        hbm = pl.BlockSpec(memory_space=pltpu.HBM)
        vmem = pl.BlockSpec(memory_space=pltpu.VMEM)
        dma = pltpu.SemaphoreType.DMA
        summed = pl.pallas_call(
            functools.partial(window_kernel, dims),
            out_shape=jax.ShapeDtypeStruct((2, depth, rows, cols), f32),
            in_specs=[hbm] * 8,
            out_specs=vmem,
            scratch_shapes=[
                pltpu.VMEM((2, 2, 3, depth, padded, cols), f32),
                pltpu.VMEM((2, 2, 2, 3, 2, padded, cols), f32),
                pltpu.VMEM((mids, 2, 2, 3, padded, cols), f32),
                pltpu.VMEM((2, 2, 3, padded, cols), f32),
                pltpu.VMEM((2, 6, depth, padded, cols), f32),
                pltpu.VMEM((2, 2, 6, padded, cols), f32),
                pltpu.VMEM((2, 3, rows, cols), f32),
                pltpu.VMEM((3, depth, rows, cols), f32),
                pltpu.VMEM((2, 3, rows, cols), f32),
                pltpu.VMEM((3, rows, cols), f32),
                pltpu.VMEM((depth + 3, rows, cols), f32),
                pltpu.VMEM((steps, depth + 2, rows, cols), f32),
                pltpu.VMEM((2, depth, rows, cols), f32),
                pltpu.VMEM((2, rows, cols), f32),
                pltpu.VMEM((2, depth, rows, cols), f32),
                pltpu.VMEM((2, depth, rows, cols), f32),
                pltpu.VMEM((2, 2, depth, rows, cols), f32),
                pltpu.SMEM(s_depth.shape, jnp.int32),
                pltpu.SMEM(s_column.shape, jnp.int32),
                pltpu.SMEM(wavelet.shape, f32),
                pltpu.VMEM(r_depth.shape, jnp.int32),
                pltpu.VMEM(r_column.shape, jnp.int32),
                pltpu.VMEM(traces.shape, f32),
                dma((3,)),
                dma((6,)),
                dma((2, 6)),
                dma((2, 6)),
                dma((2, 2, 2)),
                dma((2, 2, 2)),
                dma((mids, 2, 2)),
                dma((mids, 2, 2)),
                dma((2, 2, 2)),
                dma((2, 2, 2)),
            ],
            compiler_params=pltpu.CompilerParams(collective_id=0, has_side_effects=True),
        )(wavefields[0], earth, s_depth, s_column, wavelet, r_depth, r_column, traces)
        return summed / steps

    sharded = P(("parts", "shot"))
    return jax.shard_map(
        on_device,
        mesh=mesh,
        in_specs=(
            P(("parts", "shot"), None, None, "gz", None, None),
            P("parts", "gz", None, None),
            sharded,
            sharded,
            P(("parts", "shot"), None),
            P(("parts", "shot"), None),
            P(("parts", "shot"), None),
            P(("parts", "shot"), None, None),
        ),
        out_specs=P("parts", "gz", None, None),
        check_vma=False,
    )
```

```python
import functools
import itertools

import jax
import jax.numpy as jnp
from jax import lax
from jax.experimental import pallas as pl
from jax.experimental.pallas import tpu as pltpu
from jax.sharding import PartitionSpec as P

MESH = pl.DeviceIdType.MESH
time_step = 0.15
GUARD = 8
SXX, SYY, SZZ, SXY, SXZ, SYZ = range(6)


def window_kernel(
    dims,
    fields_in,
    earth_in,
    source_depth_in,
    source_column_in,
    wavelet_in,
    receiver_depth_in,
    receiver_column_in,
    traces_in,
    out,
    vel,
    vel_msg,
    vel_mid,
    vel_near,
    sig,
    sig_near,
    sig_far,
    mat,
    mat_near,
    mat_far,
    source_at,
    inject,
    press,
    spin,
    image,
    parts,
    source_depth,
    source_column,
    wavelet,
    receiver_depth,
    receiver_column,
    traces,
    load_sem,
    small_sem,
    keep_sem,
    first_send,
    first_recv,
    msg_send,
    msg_recv,
    mid_send,
    mid_recv,
    sum_send,
    sum_recv,
):
    slabs, shots, depth, rows, cols, steps, receivers = dims
    here = lax.axis_index("gz")
    shot = lax.axis_index("shot")
    has_up, has_down = here > 0, here < slabs - 1
    last = depth - 1
    whole = pl.ds(0, rows)
    body = pl.ds(GUARD, rows)
    after = pl.ds(GUARD + 1, rows)
    before = pl.ds(GUARD - 1, rows)
    lane = lax.broadcasted_iota(jnp.int32, (rows, cols), 1)
    row = lax.broadcasted_iota(jnp.int32, (rows, cols), 0)
    at_first, at_last = lane == 0, lane == cols - 1

    def b_y(f):
        return f - jnp.where(at_first, 0.0, pltpu.roll(f, 1, 1))

    def f_y(f):
        return jnp.where(at_last, 0.0, pltpu.roll(f, cols - 1, 1)) - f

    loads = [
        pltpu.make_async_copy(
            fields_in.at[:, 3:9], sig.at[:, :, :, body, :], load_sem.at[0]
        ),
        pltpu.make_async_copy(
            fields_in.at[:, 0:3], vel.at[1, :, :, :, body, :], load_sem.at[1]
        ),
        pltpu.make_async_copy(earth_in, mat, load_sem.at[2]),
    ]
    small = [
        pltpu.make_async_copy(src, dst, small_sem.at[i])
        for i, (src, dst) in enumerate(
            (
                (source_depth_in, source_depth),
                (source_column_in, source_column),
                (wavelet_in, wavelet),
                (receiver_depth_in, receiver_depth),
                (receiver_column_in, receiver_column),
                (traces_in, traces),
            )
        )
    ]
    for copy in loads + small:
        copy.start()

    barrier = pltpu.get_barrier_semaphore()

    def up_to(where, then):
        @pl.when(where)
        def _():
            then()

    def greet(**to):
        pl.semaphore_signal(barrier, inc=1, device_id=to, device_id_type=MESH)

    up_to(has_down, lambda: greet(gz=here + 1))
    up_to(has_up, lambda: greet(gz=here - 1))
    others = range(1, shots)
    for hop in others:
        greet(shot=lax.rem(shot + hop, shots))
    pl.semaphore_wait(barrier, shots - 1 + jnp.where(has_up, 1, 0) + jnp.where(has_down, 1, 0))

    def remote(src, dst, send, recv, **to):
        return pltpu.make_async_remote_copy(
            src_ref=src, dst_ref=dst, send_sem=send, recv_sem=recv, device_id=to, device_id_type=MESH
        )

    downs = (
        (sig.at[:, 4:6, last, body, :], sig_near.at[0, :, 4:6, body, :]),
        (fields_in.at[:, 3:7, last], sig_near.at[0, :, 0:4, body, :]),
        (fields_in.at[:, 7:9, last - 1], sig_far.at[:, 0:2]),
        (earth_in.at[:, last], mat_near.at[0]),
        (earth_in.at[2, last - 1], mat_far.at[0]),
    )
    ups = (
        (sig.at[:, 2:3, 0, body, :], sig_near.at[1, :, 2:3, body, :]),
        (fields_in.at[:, 3:5, 0], sig_near.at[1, :, 0:2, body, :]),
        (fields_in.at[:, 6:9, 0], sig_near.at[1, :, 3:6, body, :]),
        (fields_in.at[:, 5, 1], sig_far.at[:, 2]),
        (earth_in.at[:, 0], mat_near.at[1]),
        (earth_in.at[1:3, 1], mat_far.at[1:3]),
    )
    first_down = [
        remote(src, dst, first_send.at[0, i], first_recv.at[0, i], gz=here + 1)
        for i, (src, dst) in enumerate(downs)
    ]
    first_up = [
        remote(src, dst, first_send.at[1, i], first_recv.at[1, i], gz=here - 1)
        for i, (src, dst) in enumerate(ups)
    ]
    loads[0].wait()
    up_to(has_down, first_down[0].start)
    up_to(has_up, first_up[0].start)
    up_to(has_down, lambda: [copy.start() for copy in first_down[1:]])
    up_to(has_up, lambda: [copy.start() for copy in first_up[1:]])

    zeros = jnp.zeros((GUARD, cols), jnp.float32)

    def clear_around(ref, *extents):
        for index in itertools.product(*[range(extent) for extent in extents]):
            ref[(*index, pl.ds(0, GUARD), slice(None))] = zeros
            ref[(*index, pl.ds(GUARD + rows, GUARD), slice(None))] = zeros

    clear_around(sig, 2, 6, depth)
    clear_around(vel, 2, 2, 3, depth)
    clear_around(vel_near, 2, 2, 3)
    clear_around(vel_msg, 2, 2, 2, 3, 2)
    clear_around(vel_mid, steps // 2 - 1, 2, 2, 3)
    clear_around(sig_near, 2, 2, 6)

    def outside(side):
        far = pl.ds(0, 2) if side == 0 else pl.ds(2, 1)
        for view in (
            vel_msg.at[:, side, :, :, :, body, :],
            vel_mid.at[:, side, :, :, body, :],
            sig_near.at[side, :, :, body, :],
            sig_far.at[:, far],
            mat_near.at[side],
            mat_far.at[pl.ds(side, 1 + side)],
        ):
            view[...] = jnp.zeros(view.shape, jnp.float32)

    up_to(here == 0, lambda: outside(0))
    up_to(here == slabs - 1, lambda: outside(1))

    def message(w, slot, side):
        planes = pl.ds(depth - 2, 2) if side == 0 else pl.ds(0, 2)
        return remote(
            vel.at[0, w, :, planes, body, :],
            vel_msg.at[slot, side, w, :, :, body, :],
            msg_send.at[slot, side, w],
            msg_recv.at[slot, side, w],
            gz=here + 1 if side == 0 else here - 1,
        )

    def middle(w, cycle, side):
        return remote(
            vel.at[1, w, :, depth - 2 if side == 0 else 1, body, :],
            vel_mid.at[cycle, side, w, :, body, :],
            mid_send.at[cycle, side, w],
            mid_recv.at[cycle, side, w],
            gz=here + 1 if side == 0 else here - 1,
        )

    goes = (has_down, has_up)
    comes = (has_up, has_down)

    for copy in small:
        copy.wait()
    source_row = (source_depth[0] - here * depth + 1) * rows + source_column[0] // cols
    source_col = source_column[0] % cols
    for z in range(depth + 3):
        hit = (row + z * rows == source_row) & (lane == source_col)
        source_at[z] = jnp.where(hit, time_step, 0.0)
    cells = (depth + 2) * rows
    receiver_row = (receiver_depth[...] - here * depth + 1) * rows + receiver_column[...] // cols
    receiver_col = receiver_column[...] % cols
    twice_row = jnp.concatenate([receiver_row, receiver_row], axis=1)
    twice_col = jnp.concatenate([receiver_col, receiver_col], axis=1)
    in_row = lax.broadcasted_iota(jnp.int32, (cells, 2 * receivers), 0) == twice_row
    in_col = lax.broadcasted_iota(jnp.int32, (cols, 2 * receivers), 0) == twice_col
    in_col = jnp.where(in_col, 1.0, 0.0).astype(jnp.bfloat16)
    in_col = jnp.concatenate([in_col, in_col], axis=1)

    def in_bf16(f):
        return f.astype(jnp.bfloat16).astype(jnp.float32)

    amounts = time_step * traces[0]
    high = in_bf16(amounts)
    middle_part = in_bf16(amounts - high)
    low = in_bf16((amounts - high) - middle_part)
    parts[0] = jnp.concatenate([high, middle_part], axis=1)
    parts[1] = jnp.concatenate([low, jnp.zeros_like(low)], axis=1)

    def receivers_at(n, carry):
        spread = [
            jnp.where(in_row, parts[i, pl.ds(n, 1), :], 0.0).astype(jnp.bfloat16) for i in range(2)
        ]
        inject[n] = lax.dot_general(
            jnp.concatenate(spread, axis=1),
            in_col,
            (((1,), (1,)), ((), ())),
            preferred_element_type=jnp.float32,
        ).reshape(depth + 2, rows, cols)
        return carry

    lax.fori_loop(0, steps, receivers_at, 0)
    image[...] = jnp.zeros_like(image)

    for copy in loads[1:]:
        copy.wait()
    mat[...] = time_step * mat[...]

    def v(parity, slot, w, c, e, at=body):
        if 0 <= e < depth:
            return vel[parity, w, c, e, at, :]
        side = 0 if e < 0 else 1
        if parity == 0:
            return vel_msg[slot, side, w, c, e + 2 if e < 0 else e - depth, at, :]
        if e in (-1, depth):
            return vel_near[side, w, c, at, :]
        return vel_mid[slot, side, w, c, at, :]

    def s_at(w, f, e):
        if 0 <= e < depth:
            return sig, (w, f, e), True
        if e in (-1, depth):
            return sig_near, (0 if e < 0 else 1, w, f), True
        return sig_far, (w, {SXZ: 0, SYZ: 1, SZZ: 2}[f]), False

    def s(w, f, e, at=body):
        ref, index, guarded = s_at(w, f, e)
        return ref[(*index, at if guarded else whole, slice(None))]

    def add_s(w, f, e, change):
        ref, index, guarded = s_at(w, f, e)
        value = ref[(*index, body if guarded else whole, slice(None))] + change
        ref[(*index, body if guarded else whole, slice(None))] = value
        return value

    def m(which, e):
        if 0 <= e < depth:
            return mat[which, e]
        if e in (-1, depth):
            return mat_near[0 if e < 0 else 1, which]
        return mat_far[0 if e < 0 else which]

    def velocity(w, e, n, old, slot, parts_of=(0, 1, 2)):
        sxz, syz = s(w, SXZ, e), s(w, SYZ, e)
        if 0 in parts_of or 1 in parts_of:
            sxx, syy, sxy = s(w, SXX, e), s(w, SYY, e), s(w, SXY, e)
        forces = {}
        if 0 in parts_of:
            forces[0] = (s(w, SXX, e, after) - sxx) + b_y(sxy) + (sxz - s(w, SXZ, e - 1))
        if 1 in parts_of:
            forces[1] = (sxy - s(w, SXY, e, before)) + f_y(syy) + (syz - s(w, SYZ, e - 1))
        if 2 in parts_of:
            up = s(w, SZZ, e + 1) - s(w, SZZ, e)
            forces[2] = (sxz - s(w, SXZ, e, before)) + b_y(syz) + up
        buoyancy = m(0, e)
        for c, force in forces.items():
            moved = v(old, slot, w, c, e) + buoyancy * force
            if c == 2 and w == 1:
                moved = moved + inject[n, e + 1]
            if 0 <= e < depth:
                vel[1 - old, w, c, e, body, :] = moved
            else:
                vel_near[0 if e < 0 else 1, w, c, body, :] = moved

    def normal(parity, slot, w, e, n, spun=None, z_only=False):
        vx, vy, vz = [v(parity, slot, w, c, e) for c in range(3)]
        ex = vx - v(parity, slot, w, 0, e, before)
        ey = b_y(vy)
        ez = vz - v(parity, slot, w, 2, e - 1)
        common = m(1, e) * (ex + ey + ez)
        twice = 2.0 * m(2, e)
        if w == 0:
            common = common + source_at[e + 1] * wavelet[0, n]
        szz = add_s(w, SZZ, e, common + twice * ez)
        if z_only:
            return
        sxx = add_s(w, SXX, e, common + twice * ex)
        syy = add_s(w, SYY, e, common + twice * ey)
        if not 0 <= e < depth:
            return
        pressure = (sxx + syy + szz) * (1.0 / 3.0)
        if w == 0:
            press[parity, e] = pressure
        else:
            image[0, e] = image[0, e] + press[parity, e] * pressure
            if spun is not None:
                image[1, e] = image[1, e] + press[parity, e] * spin[spun]

    def shear(parity, slot, w, e, spun=None):
        vx, vy, vz = [v(parity, slot, w, c, e) for c in range(3)]
        x_up = v(parity, slot, w, 0, e + 1) - vx
        y_up = v(parity, slot, w, 1, e + 1) - vy
        z_along_x = v(parity, slot, w, 2, e, after) - vz
        z_along_y = f_y(vz)
        x_along_y = f_y(vx)
        y_along_x = v(parity, slot, w, 1, e, after) - vy
        mu = m(2, e)
        add_s(w, SXY, e, mu * (x_along_y + y_along_x))
        add_s(w, SXZ, e, mu * (x_up + z_along_x))
        add_s(w, SYZ, e, mu * (y_up + z_along_y))
        if w == 1:
            rotation = (z_along_y - y_up) + (x_up - z_along_x) + (y_along_x - x_along_y)
            if spun is None:
                image[1, e] = image[1, e] + press[parity, e] * rotation
            else:
                spin[spun] = rotation

    def shear_flat(parity, slot, w, e):
        x_along_y = f_y(v(parity, slot, w, 0, e))
        y_along_x = v(parity, slot, w, 1, e, after) - v(parity, slot, w, 1, e)
        add_s(w, SXY, e, m(2, e) * (x_along_y + y_along_x))

    def shear_deep(parity, slot, w, e):
        vx, vy, vz = [v(parity, slot, w, c, e) for c in range(3)]
        mu = m(2, e)
        z_along_x = v(parity, slot, w, 2, e, after) - vz
        add_s(w, SXZ, e, mu * ((v(parity, slot, w, 0, e + 1) - vx) + z_along_x))
        add_s(w, SYZ, e, mu * ((v(parity, slot, w, 1, e + 1) - vy) + f_y(vz)))

    def inside(cycle, n, send):
        for w in range(2):
            for e in range(1, depth):
                normal(0, None, w, e, n)
            shear(0, None, w, 0, spun=0)
            for e in range(1, last):
                shear(0, None, w, e)
            for e in (1, 2):
                velocity(w, e, n + 1, 0, None)

            def start(w=w):
                for side in range(2):
                    up_to(goes[side], middle(w, cycle, side).start)

            if send is True:
                start()
            else:
                up_to(send, start)
            normal(1, None, w, 2, n + 1)
            shear(1, None, w, 1, spun=1)

    def lower(slot, w, n, final):
        up_to(comes[1], message(w, slot, 1).wait_recv)
        shear(0, slot, w, last)
        normal(0, slot, w, depth, n)
        shear_flat(0, slot, w, depth)
        shear_deep(0, slot, w, depth)
        if not final:
            normal(0, slot, w, depth + 1, n, z_only=True)
        velocity(w, last, n + 1, 0, slot)
        velocity(w, depth, n + 1, 0, slot, (0, 1) if final else (0, 1, 2))
        normal(1, slot, w, last, n + 1)
        shear(1, slot, w, last - 1)
        shear(1, slot, w, last)
        up_to(goes[0], message(w, slot, 0).wait_send)
        if final:
            return
        normal(1, slot, w, depth, n + 1)
        velocity(w, last, n + 2, 1, slot)
        velocity(w, last - 1, n + 2, 1, slot)
        up_to(goes[0], message(w, 1 - slot, 0).start)
        shear_flat(1, slot, w, depth)

    def upper(slot, w, n, final):
        up_to(comes[0], message(w, slot, 0).wait_recv)
        normal(0, slot, w, 0, n, spun=0)
        shear_deep(0, slot, w, -1)
        normal(0, slot, w, -1, n, z_only=final)
        if not final:
            shear_flat(0, slot, w, -1)
            shear_deep(0, slot, w, -2)
        velocity(w, 0, n + 1, 0, slot)
        velocity(w, -1, n + 1, 0, slot, (2,) if final else (0, 1, 2))
        normal(1, slot, w, 0, n + 1)
        normal(1, slot, w, 1, n + 1, spun=1)
        shear(1, slot, w, 0)
        up_to(goes[1], message(w, slot, 1).wait_send)
        if final:
            return
        shear_deep(1, slot, w, -1)
        velocity(w, 0, n + 2, 1, slot)
        velocity(w, 1, n + 2, 1, slot)
        up_to(goes[1], message(w, 1 - slot, 1).start)
        shear_flat(1, slot, w, -1)

    def catch_up(cycle, n):
        for w in range(2):
            up_to(comes[1], middle(w, cycle, 1).wait_recv)
            shear_deep(1, cycle, w, depth)
            normal(1, cycle, w, depth + 1, n, z_only=True)
            up_to(comes[0], middle(w, cycle, 0).wait_recv)
            normal(1, cycle, w, -1, n)
            shear_deep(1, cycle, w, -2)

    up_to(comes[1], first_up[0].wait_recv)
    for w in range(2):
        velocity(w, last, 0, 1, None)
        velocity(w, last - 1, 0, 1, None)
        up_to(goes[0], message(w, 0, 0).start)
    up_to(comes[0], first_down[0].wait_recv)
    for w in range(2):
        velocity(w, 0, 0, 1, None)
        velocity(w, 1, 0, 1, None)
        up_to(goes[1], message(w, 0, 1).start)
    inside(0, 0, True)
    up_to(comes[1], lambda: [copy.wait_recv() for copy in first_up[1:]])
    up_to(comes[0], lambda: [copy.wait_recv() for copy in first_down[1:]])
    mat_near[...] = time_step * mat_near[...]
    mat_far[...] = time_step * mat_far[...]

    up_to(has_down, first_down[0].wait_send)
    up_to(has_up, first_up[0].wait_send)

    cycles = steps // 2

    def cycle_body(cycle, carry):
        slot = lax.rem(cycle, 2)
        n = 2 * cycle
        for w in range(2):
            lower(slot, w, n, False)
        for w in range(2):
            upper(slot, w, n, False)
        for w in range(2):
            for side in range(2):
                up_to(goes[side], middle(w, cycle, side).wait_send)
        inside(cycle + 1, n + 2, cycle < cycles - 2)
        catch_up(cycle, n + 1)
        return carry

    lax.fori_loop(0, cycles - 1, cycle_body, 0)

    def to_shot(half, hop, source):
        planes = pl.ds(2 * half, 2)
        return remote(
            image.at[:, planes],
            out.at[source, :, planes],
            sum_send.at[half, hop],
            sum_recv.at[half, hop],
            shot=lax.rem(shot + hop, shots),
        )

    def keep(half):
        planes = pl.ds(2 * half, 2)
        return pltpu.make_async_copy(image.at[:, planes], out.at[shot, :, planes], keep_sem.at[half])

    def hand_over(half):
        for hop in (2, 1, 3):
            to_shot(half, hop, shot).start()
        keep(half).start()

    end = (cycles - 1) % 2
    for w in range(2):
        lower(end, w, steps - 2, True)
    hand_over(1)
    for w in range(2):
        upper(end, w, steps - 2, True)
    hand_over(0)
    up_to(has_down, lambda: [copy.wait_send() for copy in first_down[1:]])
    up_to(has_up, lambda: [copy.wait_send() for copy in first_up[1:]])
    for half in (1, 0):
        keep(half).wait()
        for hop in others:
            to_shot(half, hop, lax.rem(shot + shots - hop, shots)).wait_recv()
    for half in (1, 0):
        for hop in others:
            to_shot(half, hop, shot).wait_send()


def solution(mesh):
    slabs, shots = mesh.shape["gz"], mesh.shape["shot"]

    def on_device(wavefields, earth, s_depth, s_column, wavelet, r_depth, r_column, traces):
        depth, rows, cols = earth.shape[1:]
        steps, receivers = traces.shape[1:]
        assert depth == 4 and shots == 4 and steps % 2 == 0 and steps >= 4
        dims = (slabs, shots, depth, rows, cols, steps, receivers)
        padded = rows + 2 * GUARD
        f32 = jnp.float32
        mids = steps // 2 - 1
        hbm = pl.BlockSpec(memory_space=pltpu.HBM)
        dma = pltpu.SemaphoreType.DMA
        by_shot = pl.pallas_call(
            functools.partial(window_kernel, dims),
            out_shape=jax.ShapeDtypeStruct((shots, 2, depth, rows, cols), f32),
            in_specs=[hbm] * 8,
            out_specs=hbm,
            scratch_shapes=[
                pltpu.VMEM((2, 2, 3, depth, padded, cols), f32),
                pltpu.VMEM((2, 2, 2, 3, 2, padded, cols), f32),
                pltpu.VMEM((mids, 2, 2, 3, padded, cols), f32),
                pltpu.VMEM((2, 2, 3, padded, cols), f32),
                pltpu.VMEM((2, 6, depth, padded, cols), f32),
                pltpu.VMEM((2, 2, 6, padded, cols), f32),
                pltpu.VMEM((2, 3, rows, cols), f32),
                pltpu.VMEM((3, depth, rows, cols), f32),
                pltpu.VMEM((2, 3, rows, cols), f32),
                pltpu.VMEM((3, rows, cols), f32),
                pltpu.VMEM((depth + 3, rows, cols), f32),
                pltpu.VMEM((steps, depth + 2, rows, cols), f32),
                pltpu.VMEM((2, depth, rows, cols), f32),
                pltpu.VMEM((2, rows, cols), f32),
                pltpu.VMEM((2, depth, rows, cols), f32),
                pltpu.VMEM((2, steps, 2 * receivers), f32),
                pltpu.SMEM(s_depth.shape, jnp.int32),
                pltpu.SMEM(s_column.shape, jnp.int32),
                pltpu.SMEM(wavelet.shape, f32),
                pltpu.VMEM(r_depth.shape, jnp.int32),
                pltpu.VMEM(r_column.shape, jnp.int32),
                pltpu.VMEM(traces.shape, f32),
                dma((3,)),
                dma((6,)),
                dma((2,)),
                dma((2, 6)),
                dma((2, 6)),
                dma((2, 2, 2)),
                dma((2, 2, 2)),
                dma((mids, 2, 2)),
                dma((mids, 2, 2)),
                dma((2, shots)),
                dma((2, shots)),
            ],
            compiler_params=pltpu.CompilerParams(
                collective_id=0, has_side_effects=True
            ),
        )(wavefields[0], earth, s_depth, s_column, wavelet, r_depth, r_column, traces)
        return sum(by_shot[i] for i in range(1, shots)) / steps + by_shot[0] / steps

    sharded = P(("parts", "shot"))
    return jax.shard_map(
        on_device,
        mesh=mesh,
        in_specs=(
            P(("parts", "shot"), None, None, "gz", None, None),
            P("parts", "gz", None, None),
            sharded,
            sharded,
            P(("parts", "shot"), None),
            P(("parts", "shot"), None),
            P(("parts", "shot"), None),
            P(("parts", "shot"), None, None),
        ),
        out_specs=P("parts", "gz", None, None),
        check_vma=False,
    )
```

```python
import functools
import itertools

import jax
import jax.numpy as jnp
from jax import lax
from jax.experimental import pallas as pl
from jax.experimental.pallas import tpu as pltpu
from jax.sharding import PartitionSpec as P

MESH = pl.DeviceIdType.MESH
time_step = 0.15
GUARD = 8
SXX, SYY, SZZ, SXY, SXZ, SYZ = range(6)


def window_kernel(
    dims,
    fields_in,
    earth_in,
    source_depth_in,
    source_column_in,
    wavelet_in,
    receiver_depth_in,
    receiver_column_in,
    traces_in,
    out,
    vel,
    vel_msg,
    vel_mid,
    vel_near,
    sig,
    sig_near,
    sig_far,
    mat,
    mat_near,
    mat_far,
    source_at,
    inject,
    press,
    spin,
    image,
    partial,
    landed,
    parts,
    source_depth,
    source_column,
    wavelet,
    receiver_depth,
    receiver_column,
    traces,
    load_sem,
    small_sem,
    keep_sem,
    first_send,
    first_recv,
    msg_send,
    msg_recv,
    mid_send,
    mid_recv,
    sum_send,
    sum_recv,
):
    slabs, shots, depth, rows, cols, steps, receivers = dims
    here = lax.axis_index("gz")
    shot = lax.axis_index("shot")
    has_up, has_down = here > 0, here < slabs - 1
    last = depth - 1
    whole = pl.ds(0, rows)
    body = pl.ds(GUARD, rows)
    after = pl.ds(GUARD + 1, rows)
    before = pl.ds(GUARD - 1, rows)
    lane = lax.broadcasted_iota(jnp.int32, (rows, cols), 1)
    row = lax.broadcasted_iota(jnp.int32, (rows, cols), 0)
    at_first, at_last = lane == 0, lane == cols - 1

    def b_y(f):
        return f - jnp.where(at_first, 0.0, pltpu.roll(f, 1, 1))

    def f_y(f):
        return jnp.where(at_last, 0.0, pltpu.roll(f, cols - 1, 1)) - f

    loads = [
        pltpu.make_async_copy(
            fields_in.at[:, 3:9], sig.at[:, :, :, body, :], load_sem.at[0]
        ),
        pltpu.make_async_copy(
            fields_in.at[:, 0:3], vel.at[1, :, :, :, body, :], load_sem.at[1]
        ),
        pltpu.make_async_copy(earth_in, mat, load_sem.at[2]),
    ]
    small = [
        pltpu.make_async_copy(src, dst, small_sem.at[i])
        for i, (src, dst) in enumerate(
            (
                (source_depth_in, source_depth),
                (source_column_in, source_column),
                (wavelet_in, wavelet),
                (receiver_depth_in, receiver_depth),
                (receiver_column_in, receiver_column),
                (traces_in, traces),
            )
        )
    ]
    for copy in loads + small:
        copy.start()

    barrier = pltpu.get_barrier_semaphore()

    def up_to(where, then):
        @pl.when(where)
        def _():
            then()

    def greet(**to):
        pl.semaphore_signal(barrier, inc=1, device_id=to, device_id_type=MESH)

    up_to(has_down, lambda: greet(gz=here + 1))
    up_to(has_up, lambda: greet(gz=here - 1))
    partners = (shot + 1 - 2 * lax.rem(shot, 2), shots - 1 - shot)
    for partner in partners:
        greet(shot=partner)
    pl.semaphore_wait(barrier, 2 + jnp.where(has_up, 1, 0) + jnp.where(has_down, 1, 0))

    def remote(src, dst, send, recv, **to):
        return pltpu.make_async_remote_copy(
            src_ref=src, dst_ref=dst, send_sem=send, recv_sem=recv, device_id=to, device_id_type=MESH
        )

    downs = (
        (sig.at[:, 4:6, last, body, :], sig_near.at[0, :, 4:6, body, :]),
        (fields_in.at[:, 3:7, last], sig_near.at[0, :, 0:4, body, :]),
        (fields_in.at[:, 7:9, last - 1], sig_far.at[:, 0:2]),
        (earth_in.at[:, last], mat_near.at[0]),
        (earth_in.at[2, last - 1], mat_far.at[0]),
    )
    ups = (
        (sig.at[:, 2:3, 0, body, :], sig_near.at[1, :, 2:3, body, :]),
        (fields_in.at[:, 3:5, 0], sig_near.at[1, :, 0:2, body, :]),
        (fields_in.at[:, 6:9, 0], sig_near.at[1, :, 3:6, body, :]),
        (fields_in.at[:, 5, 1], sig_far.at[:, 2]),
        (earth_in.at[:, 0], mat_near.at[1]),
        (earth_in.at[1:3, 1], mat_far.at[1:3]),
    )
    first_down = [
        remote(src, dst, first_send.at[0, i], first_recv.at[0, i], gz=here + 1)
        for i, (src, dst) in enumerate(downs)
    ]
    first_up = [
        remote(src, dst, first_send.at[1, i], first_recv.at[1, i], gz=here - 1)
        for i, (src, dst) in enumerate(ups)
    ]
    loads[0].wait()
    up_to(has_down, first_down[0].start)
    up_to(has_up, first_up[0].start)
    up_to(has_down, lambda: [copy.start() for copy in first_down[1:]])
    up_to(has_up, lambda: [copy.start() for copy in first_up[1:]])

    zeros = jnp.zeros((GUARD, cols), jnp.float32)

    def clear_around(ref, *extents):
        for index in itertools.product(*[range(extent) for extent in extents]):
            ref[(*index, pl.ds(0, GUARD), slice(None))] = zeros
            ref[(*index, pl.ds(GUARD + rows, GUARD), slice(None))] = zeros

    clear_around(sig, 2, 6, depth)
    clear_around(vel, 2, 2, 3, depth)
    clear_around(vel_near, 2, 2, 3)
    clear_around(vel_msg, 2, 2, 2, 3, 2)
    clear_around(vel_mid, steps // 2 - 1, 2, 2, 3)
    clear_around(sig_near, 2, 2, 6)

    def outside(side):
        far = pl.ds(0, 2) if side == 0 else pl.ds(2, 1)
        for view in (
            vel_msg.at[:, side, :, :, :, body, :],
            vel_mid.at[:, side, :, :, body, :],
            sig_near.at[side, :, :, body, :],
            sig_far.at[:, far],
            mat_near.at[side],
            mat_far.at[pl.ds(side, 1 + side)],
        ):
            view[...] = jnp.zeros(view.shape, jnp.float32)

    up_to(here == 0, lambda: outside(0))
    up_to(here == slabs - 1, lambda: outside(1))

    def message(w, slot, side):
        planes = pl.ds(depth - 2, 2) if side == 0 else pl.ds(0, 2)
        return remote(
            vel.at[0, w, :, planes, body, :],
            vel_msg.at[slot, side, w, :, :, body, :],
            msg_send.at[slot, side, w],
            msg_recv.at[slot, side, w],
            gz=here + 1 if side == 0 else here - 1,
        )

    def middle(w, cycle, side):
        return remote(
            vel.at[1, w, :, depth - 2 if side == 0 else 1, body, :],
            vel_mid.at[cycle, side, w, :, body, :],
            mid_send.at[cycle, side, w],
            mid_recv.at[cycle, side, w],
            gz=here + 1 if side == 0 else here - 1,
        )

    goes = (has_down, has_up)
    comes = (has_up, has_down)

    for copy in small:
        copy.wait()
    source_row = (source_depth[0] - here * depth + 1) * rows + source_column[0] // cols
    source_col = source_column[0] % cols
    for z in range(depth + 3):
        hit = (row + z * rows == source_row) & (lane == source_col)
        source_at[z] = jnp.where(hit, time_step, 0.0)
    cells = (depth + 2) * rows
    receiver_row = (receiver_depth[...] - here * depth + 1) * rows + receiver_column[...] // cols
    receiver_col = receiver_column[...] % cols
    twice_row = jnp.concatenate([receiver_row, receiver_row], axis=1)
    twice_col = jnp.concatenate([receiver_col, receiver_col], axis=1)
    in_row = lax.broadcasted_iota(jnp.int32, (cells, 2 * receivers), 0) == twice_row
    in_col = lax.broadcasted_iota(jnp.int32, (cols, 2 * receivers), 0) == twice_col
    in_col = jnp.where(in_col, 1.0, 0.0).astype(jnp.bfloat16)
    in_col = jnp.concatenate([in_col, in_col], axis=1)

    def in_bf16(f):
        return f.astype(jnp.bfloat16).astype(jnp.float32)

    amounts = time_step * traces[0]
    high = in_bf16(amounts)
    middle_part = in_bf16(amounts - high)
    low = in_bf16((amounts - high) - middle_part)
    parts[0] = jnp.concatenate([high, middle_part], axis=1)
    parts[1] = jnp.concatenate([low, jnp.zeros_like(low)], axis=1)

    def receivers_at(n, carry):
        spread = [
            jnp.where(in_row, parts[i, pl.ds(n, 1), :], 0.0).astype(jnp.bfloat16) for i in range(2)
        ]
        inject[n] = lax.dot_general(
            jnp.concatenate(spread, axis=1),
            in_col,
            (((1,), (1,)), ((), ())),
            preferred_element_type=jnp.float32,
        ).reshape(depth + 2, rows, cols)
        return carry

    lax.fori_loop(0, steps, receivers_at, 0)
    image[...] = jnp.zeros_like(image)

    for copy in loads[1:]:
        copy.wait()
    mat[...] = time_step * mat[...]

    def v(parity, slot, w, c, e, at=body):
        if 0 <= e < depth:
            return vel[parity, w, c, e, at, :]
        side = 0 if e < 0 else 1
        if parity == 0:
            return vel_msg[slot, side, w, c, e + 2 if e < 0 else e - depth, at, :]
        if e in (-1, depth):
            return vel_near[side, w, c, at, :]
        return vel_mid[slot, side, w, c, at, :]

    def s_at(w, f, e):
        if 0 <= e < depth:
            return sig, (w, f, e), True
        if e in (-1, depth):
            return sig_near, (0 if e < 0 else 1, w, f), True
        return sig_far, (w, {SXZ: 0, SYZ: 1, SZZ: 2}[f]), False

    def s(w, f, e, at=body):
        ref, index, guarded = s_at(w, f, e)
        return ref[(*index, at if guarded else whole, slice(None))]

    def add_s(w, f, e, change):
        ref, index, guarded = s_at(w, f, e)
        value = ref[(*index, body if guarded else whole, slice(None))] + change
        ref[(*index, body if guarded else whole, slice(None))] = value
        return value

    def m(which, e):
        if 0 <= e < depth:
            return mat[which, e]
        if e in (-1, depth):
            return mat_near[0 if e < 0 else 1, which]
        return mat_far[0 if e < 0 else which]

    def velocity(w, e, n, old, slot, parts_of=(0, 1, 2)):
        sxz, syz = s(w, SXZ, e), s(w, SYZ, e)
        if 0 in parts_of or 1 in parts_of:
            sxx, syy, sxy = s(w, SXX, e), s(w, SYY, e), s(w, SXY, e)
        forces = {}
        if 0 in parts_of:
            forces[0] = (s(w, SXX, e, after) - sxx) + b_y(sxy) + (sxz - s(w, SXZ, e - 1))
        if 1 in parts_of:
            forces[1] = (sxy - s(w, SXY, e, before)) + f_y(syy) + (syz - s(w, SYZ, e - 1))
        if 2 in parts_of:
            up = s(w, SZZ, e + 1) - s(w, SZZ, e)
            forces[2] = (sxz - s(w, SXZ, e, before)) + b_y(syz) + up
        buoyancy = m(0, e)
        for c, force in forces.items():
            moved = v(old, slot, w, c, e) + buoyancy * force
            if c == 2 and w == 1:
                moved = moved + inject[n, e + 1]
            if 0 <= e < depth:
                vel[1 - old, w, c, e, body, :] = moved
            else:
                vel_near[0 if e < 0 else 1, w, c, body, :] = moved

    def normal(parity, slot, w, e, n, spun=None, z_only=False):
        vx, vy, vz = [v(parity, slot, w, c, e) for c in range(3)]
        ex = vx - v(parity, slot, w, 0, e, before)
        ey = b_y(vy)
        ez = vz - v(parity, slot, w, 2, e - 1)
        common = m(1, e) * (ex + ey + ez)
        twice = 2.0 * m(2, e)
        if w == 0:
            common = common + source_at[e + 1] * wavelet[0, n]
        szz = add_s(w, SZZ, e, common + twice * ez)
        if z_only:
            return
        sxx = add_s(w, SXX, e, common + twice * ex)
        syy = add_s(w, SYY, e, common + twice * ey)
        if not 0 <= e < depth:
            return
        pressure = (sxx + syy + szz) * (1.0 / 3.0)
        if w == 0:
            press[parity, e] = pressure
        else:
            image[0, e] = image[0, e] + press[parity, e] * pressure
            if spun is not None:
                image[1, e] = image[1, e] + press[parity, e] * spin[spun]

    def shear(parity, slot, w, e, spun=None):
        vx, vy, vz = [v(parity, slot, w, c, e) for c in range(3)]
        x_up = v(parity, slot, w, 0, e + 1) - vx
        y_up = v(parity, slot, w, 1, e + 1) - vy
        z_along_x = v(parity, slot, w, 2, e, after) - vz
        z_along_y = f_y(vz)
        x_along_y = f_y(vx)
        y_along_x = v(parity, slot, w, 1, e, after) - vy
        mu = m(2, e)
        add_s(w, SXY, e, mu * (x_along_y + y_along_x))
        add_s(w, SXZ, e, mu * (x_up + z_along_x))
        add_s(w, SYZ, e, mu * (y_up + z_along_y))
        if w == 1:
            rotation = (z_along_y - y_up) + (x_up - z_along_x) + (y_along_x - x_along_y)
            if spun is None:
                image[1, e] = image[1, e] + press[parity, e] * rotation
            else:
                spin[spun] = rotation

    def shear_flat(parity, slot, w, e):
        x_along_y = f_y(v(parity, slot, w, 0, e))
        y_along_x = v(parity, slot, w, 1, e, after) - v(parity, slot, w, 1, e)
        add_s(w, SXY, e, m(2, e) * (x_along_y + y_along_x))

    def shear_deep(parity, slot, w, e):
        vx, vy, vz = [v(parity, slot, w, c, e) for c in range(3)]
        mu = m(2, e)
        z_along_x = v(parity, slot, w, 2, e, after) - vz
        add_s(w, SXZ, e, mu * ((v(parity, slot, w, 0, e + 1) - vx) + z_along_x))
        add_s(w, SYZ, e, mu * ((v(parity, slot, w, 1, e + 1) - vy) + f_y(vz)))

    def inside(cycle, n, send):
        for w in range(2):
            for e in range(1, depth):
                normal(0, None, w, e, n)
            shear(0, None, w, 0, spun=0)
            for e in range(1, last):
                shear(0, None, w, e)
            for e in (1, 2):
                velocity(w, e, n + 1, 0, None)

            def start(w=w):
                for side in range(2):
                    up_to(goes[side], middle(w, cycle, side).start)

            if send is True:
                start()
            else:
                up_to(send, start)
            normal(1, None, w, 2, n + 1)
            shear(1, None, w, 1, spun=1)

    def lower(slot, w, n, final):
        up_to(comes[1], message(w, slot, 1).wait_recv)
        shear(0, slot, w, last)
        normal(0, slot, w, depth, n)
        shear_flat(0, slot, w, depth)
        shear_deep(0, slot, w, depth)
        if not final:
            normal(0, slot, w, depth + 1, n, z_only=True)
        velocity(w, last, n + 1, 0, slot)
        velocity(w, depth, n + 1, 0, slot, (0, 1) if final else (0, 1, 2))
        normal(1, slot, w, last, n + 1)
        shear(1, slot, w, last - 1)
        shear(1, slot, w, last)
        up_to(goes[0], message(w, slot, 0).wait_send)
        if final:
            return
        normal(1, slot, w, depth, n + 1)
        velocity(w, last, n + 2, 1, slot)
        velocity(w, last - 1, n + 2, 1, slot)
        up_to(goes[0], message(w, 1 - slot, 0).start)
        shear_flat(1, slot, w, depth)

    def upper(slot, w, n, final):
        up_to(comes[0], message(w, slot, 0).wait_recv)
        normal(0, slot, w, 0, n, spun=0)
        shear_deep(0, slot, w, -1)
        normal(0, slot, w, -1, n, z_only=final)
        if not final:
            shear_flat(0, slot, w, -1)
            shear_deep(0, slot, w, -2)
        velocity(w, 0, n + 1, 0, slot)
        velocity(w, -1, n + 1, 0, slot, (2,) if final else (0, 1, 2))
        normal(1, slot, w, 0, n + 1)
        normal(1, slot, w, 1, n + 1, spun=1)
        shear(1, slot, w, 0)
        up_to(goes[1], message(w, slot, 1).wait_send)
        if final:
            return
        shear_deep(1, slot, w, -1)
        velocity(w, 0, n + 2, 1, slot)
        velocity(w, 1, n + 2, 1, slot)
        up_to(goes[1], message(w, 1 - slot, 1).start)
        shear_flat(1, slot, w, -1)

    def catch_up(cycle, n):
        for w in range(2):
            up_to(comes[1], middle(w, cycle, 1).wait_recv)
            shear_deep(1, cycle, w, depth)
            normal(1, cycle, w, depth + 1, n, z_only=True)
            up_to(comes[0], middle(w, cycle, 0).wait_recv)
            normal(1, cycle, w, -1, n)
            shear_deep(1, cycle, w, -2)

    up_to(comes[1], first_up[0].wait_recv)
    for w in range(2):
        velocity(w, last, 0, 1, None)
        velocity(w, last - 1, 0, 1, None)
        up_to(goes[0], message(w, 0, 0).start)
    up_to(comes[0], first_down[0].wait_recv)
    for w in range(2):
        velocity(w, 0, 0, 1, None)
        velocity(w, 1, 0, 1, None)
        up_to(goes[1], message(w, 0, 1).start)
    inside(0, 0, True)
    up_to(comes[1], lambda: [copy.wait_recv() for copy in first_up[1:]])
    up_to(comes[0], lambda: [copy.wait_recv() for copy in first_down[1:]])
    mat_near[...] = time_step * mat_near[...]
    mat_far[...] = time_step * mat_far[...]

    up_to(has_down, first_down[0].wait_send)
    up_to(has_up, first_up[0].wait_send)

    cycles = steps // 2

    def cycle_body(cycle, carry):
        slot = lax.rem(cycle, 2)
        n = 2 * cycle
        for w in range(2):
            lower(slot, w, n, False)
        for w in range(2):
            upper(slot, w, n, False)
        for w in range(2):
            for side in range(2):
                up_to(goes[side], middle(w, cycle, side).wait_send)
        inside(cycle + 1, n + 2, cycle < cycles - 2)
        catch_up(cycle, n + 1)
        return carry

    lax.fori_loop(0, cycles - 1, cycle_body, 0)

    pieces = ((2, 2), (0, 1), (1, 1))

    def first_round(piece, i):
        planes = pl.ds(*pieces[piece])
        return remote(
            image.at[i, planes],
            landed.at[i, planes],
            sum_send.at[0, piece, i],
            sum_recv.at[0, piece, i],
            shot=partners[i],
        )

    def second_round(piece, i):
        planes = pl.ds(*pieces[piece])
        return remote(
            partial.at[i, planes],
            out.at[1, i, planes],
            sum_send.at[1, piece, i],
            sum_recv.at[1, piece, i],
            shot=partners[1 - i],
        )

    def keep(piece, i):
        planes = pl.ds(*pieces[piece])
        return pltpu.make_async_copy(partial.at[i, planes], out.at[0, i, planes], keep_sem.at[piece, i])

    end = (cycles - 1) % 2
    for w in range(2):
        lower(end, w, steps - 2, True)
    for i in range(2):
        first_round(0, i).start()
    for w in range(2):
        upper(end, w, steps - 2, True)
    for piece in (1, 2):
        for i in range(2):
            first_round(piece, i).start()
    for piece in range(3):
        planes = pl.ds(*pieces[piece])
        for i in range(2):
            first_round(piece, i).wait_recv()
            partial[i, planes] = image[i, planes] + landed[i, planes]
        for i in range(2):
            second_round(piece, i).start()
            keep(piece, i).start()
    up_to(has_down, lambda: [copy.wait_send() for copy in first_down[1:]])
    up_to(has_up, lambda: [copy.wait_send() for copy in first_up[1:]])
    for piece in range(3):
        for i in range(2):
            first_round(piece, i).wait_send()
            keep(piece, i).wait()
            second_round(piece, i).wait_send()
    for piece in range(3):
        for i in range(2):
            second_round(piece, i).wait_recv()


def solution(mesh):
    slabs, shots = mesh.shape["gz"], mesh.shape["shot"]

    def on_device(wavefields, earth, s_depth, s_column, wavelet, r_depth, r_column, traces):
        depth, rows, cols = earth.shape[1:]
        steps, receivers = traces.shape[1:]
        assert depth == 4 and shots == 4 and steps % 2 == 0 and steps >= 4
        dims = (slabs, shots, depth, rows, cols, steps, receivers)
        padded = rows + 2 * GUARD
        f32 = jnp.float32
        mids = steps // 2 - 1
        hbm = pl.BlockSpec(memory_space=pltpu.HBM)
        dma = pltpu.SemaphoreType.DMA
        pairs = pl.pallas_call(
            functools.partial(window_kernel, dims),
            out_shape=jax.ShapeDtypeStruct((2, 2, depth, rows, cols), f32),
            in_specs=[hbm] * 8,
            out_specs=hbm,
            scratch_shapes=[
                pltpu.VMEM((2, 2, 3, depth, padded, cols), f32),
                pltpu.VMEM((2, 2, 2, 3, 2, padded, cols), f32),
                pltpu.VMEM((mids, 2, 2, 3, padded, cols), f32),
                pltpu.VMEM((2, 2, 3, padded, cols), f32),
                pltpu.VMEM((2, 6, depth, padded, cols), f32),
                pltpu.VMEM((2, 2, 6, padded, cols), f32),
                pltpu.VMEM((2, 3, rows, cols), f32),
                pltpu.VMEM((3, depth, rows, cols), f32),
                pltpu.VMEM((2, 3, rows, cols), f32),
                pltpu.VMEM((3, rows, cols), f32),
                pltpu.VMEM((depth + 3, rows, cols), f32),
                pltpu.VMEM((steps, depth + 2, rows, cols), f32),
                pltpu.VMEM((2, depth, rows, cols), f32),
                pltpu.VMEM((2, rows, cols), f32),
                pltpu.VMEM((2, depth, rows, cols), f32),
                pltpu.VMEM((2, depth, rows, cols), f32),
                pltpu.VMEM((2, depth, rows, cols), f32),
                pltpu.VMEM((2, steps, 2 * receivers), f32),
                pltpu.SMEM(s_depth.shape, jnp.int32),
                pltpu.SMEM(s_column.shape, jnp.int32),
                pltpu.SMEM(wavelet.shape, f32),
                pltpu.VMEM(r_depth.shape, jnp.int32),
                pltpu.VMEM(r_column.shape, jnp.int32),
                pltpu.VMEM(traces.shape, f32),
                dma((3,)),
                dma((6,)),
                dma((3, 2)),
                dma((2, 6)),
                dma((2, 6)),
                dma((2, 2, 2)),
                dma((2, 2, 2)),
                dma((mids, 2, 2)),
                dma((mids, 2, 2)),
                dma((2, 3, 2)),
                dma((2, 3, 2)),
            ],
            compiler_params=pltpu.CompilerParams(
                collective_id=0, has_side_effects=True
            ),
        )(wavefields[0], earth, s_depth, s_column, wavelet, r_depth, r_column, traces)
        return (pairs[0] + pairs[1]) / steps

    sharded = P(("parts", "shot"))
    return jax.shard_map(
        on_device,
        mesh=mesh,
        in_specs=(
            P(("parts", "shot"), None, None, "gz", None, None),
            P("parts", "gz", None, None),
            sharded,
            sharded,
            P(("parts", "shot"), None),
            P(("parts", "shot"), None),
            P(("parts", "shot"), None),
            P(("parts", "shot"), None, None),
        ),
        out_specs=P("parts", "gz", None, None),
        check_vma=False,
    )
```

```python
import functools
import itertools

import jax
import jax.numpy as jnp
from jax import lax
from jax.experimental import pallas as pl
from jax.experimental.pallas import tpu as pltpu
from jax.sharding import PartitionSpec as P

MESH = pl.DeviceIdType.MESH
time_step = 0.15
GUARD = 8
SXX, SYY, SZZ, SXY, SXZ, SYZ = range(6)


def window_kernel(
    dims,
    fields_in,
    earth_in,
    source_depth_in,
    source_column_in,
    wavelet_in,
    receiver_depth_in,
    receiver_column_in,
    traces_in,
    out,
    vel,
    vel_msg,
    vel_mid,
    vel_near,
    sig,
    sig_near,
    sig_far,
    mat,
    mat_near,
    mat_far,
    source_at,
    inject,
    press,
    spin,
    image,
    parts,
    source_depth,
    source_column,
    wavelet,
    receiver_depth,
    receiver_column,
    traces,
    load_sem,
    small_sem,
    keep_sem,
    first_send,
    first_recv,
    msg_send,
    msg_recv,
    mid_send,
    mid_recv,
    sum_send,
    sum_recv,
):
    slabs, shots, depth, rows, cols, steps, receivers = dims
    here = lax.axis_index("gz")
    shot = lax.axis_index("shot")
    has_up, has_down = here > 0, here < slabs - 1
    last = depth - 1
    whole = pl.ds(0, rows)
    body = pl.ds(GUARD, rows)
    after = pl.ds(GUARD + 1, rows)
    before = pl.ds(GUARD - 1, rows)
    lane = lax.broadcasted_iota(jnp.int32, (rows, cols), 1)
    row = lax.broadcasted_iota(jnp.int32, (rows, cols), 0)
    at_first, at_last = lane == 0, lane == cols - 1

    def b_y(f):
        return f - jnp.where(at_first, 0.0, pltpu.roll(f, 1, 1))

    def f_y(f):
        return jnp.where(at_last, 0.0, pltpu.roll(f, cols - 1, 1)) - f

    loads = [
        pltpu.make_async_copy(
            fields_in.at[:, 3:9], sig.at[:, :, :, body, :], load_sem.at[0]
        ),
        pltpu.make_async_copy(
            fields_in.at[:, 0:3], vel.at[1, :, :, :, body, :], load_sem.at[1]
        ),
        pltpu.make_async_copy(earth_in, mat, load_sem.at[2]),
    ]
    small = [
        pltpu.make_async_copy(src, dst, small_sem.at[i])
        for i, (src, dst) in enumerate(
            (
                (source_depth_in, source_depth),
                (source_column_in, source_column),
                (wavelet_in, wavelet),
                (receiver_depth_in, receiver_depth),
                (receiver_column_in, receiver_column),
                (traces_in, traces),
            )
        )
    ]
    for copy in loads + small:
        copy.start()

    barrier = pltpu.get_barrier_semaphore()

    def up_to(where, then):
        @pl.when(where)
        def _():
            then()

    def greet(**to):
        pl.semaphore_signal(barrier, inc=1, device_id=to, device_id_type=MESH)

    up_to(has_down, lambda: greet(gz=here + 1))
    up_to(has_up, lambda: greet(gz=here - 1))
    others = range(1, shots)
    for hop in others:
        greet(shot=lax.rem(shot + hop, shots))
    pl.semaphore_wait(barrier, shots - 1 + jnp.where(has_up, 1, 0) + jnp.where(has_down, 1, 0))

    def remote(src, dst, send, recv, **to):
        return pltpu.make_async_remote_copy(
            src_ref=src, dst_ref=dst, send_sem=send, recv_sem=recv, device_id=to, device_id_type=MESH
        )

    downs = (
        (sig.at[:, 4:6, last, body, :], sig_near.at[0, :, 4:6, body, :]),
        (fields_in.at[:, 3:7, last], sig_near.at[0, :, 0:4, body, :]),
        (fields_in.at[:, 7:9, last - 1], sig_far.at[:, 0:2]),
        (earth_in.at[:, last], mat_near.at[0]),
        (earth_in.at[2, last - 1], mat_far.at[0]),
    )
    ups = (
        (sig.at[:, 2:3, 0, body, :], sig_near.at[1, :, 2:3, body, :]),
        (fields_in.at[:, 3:5, 0], sig_near.at[1, :, 0:2, body, :]),
        (fields_in.at[:, 6:9, 0], sig_near.at[1, :, 3:6, body, :]),
        (fields_in.at[:, 5, 1], sig_far.at[:, 2]),
        (earth_in.at[:, 0], mat_near.at[1]),
        (earth_in.at[1:3, 1], mat_far.at[1:3]),
    )
    first_down = [
        remote(src, dst, first_send.at[0, i], first_recv.at[0, i], gz=here + 1)
        for i, (src, dst) in enumerate(downs)
    ]
    first_up = [
        remote(src, dst, first_send.at[1, i], first_recv.at[1, i], gz=here - 1)
        for i, (src, dst) in enumerate(ups)
    ]
    loads[0].wait()
    up_to(has_down, first_down[0].start)
    up_to(has_up, first_up[0].start)
    up_to(has_down, lambda: [copy.start() for copy in first_down[1:]])
    up_to(has_up, lambda: [copy.start() for copy in first_up[1:]])

    zeros = jnp.zeros((GUARD, cols), jnp.float32)

    def clear_around(ref, *extents):
        for index in itertools.product(*[range(extent) for extent in extents]):
            ref[(*index, pl.ds(0, GUARD), slice(None))] = zeros
            ref[(*index, pl.ds(GUARD + rows, GUARD), slice(None))] = zeros

    clear_around(sig, 2, 6, depth)
    clear_around(vel, 2, 2, 3, depth)
    clear_around(vel_near, 2, 2, 3)
    clear_around(vel_msg, 2, 2, 2, 3, 2)
    clear_around(vel_mid, steps // 2 - 1, 2, 2, 3)
    clear_around(sig_near, 2, 2, 6)

    def outside(side):
        far = pl.ds(0, 2) if side == 0 else pl.ds(2, 1)
        for view in (
            vel_msg.at[:, side, :, :, :, body, :],
            vel_mid.at[:, side, :, :, body, :],
            sig_near.at[side, :, :, body, :],
            sig_far.at[:, far],
            mat_near.at[side],
            mat_far.at[pl.ds(side, 1 + side)],
        ):
            view[...] = jnp.zeros(view.shape, jnp.float32)

    up_to(here == 0, lambda: outside(0))
    up_to(here == slabs - 1, lambda: outside(1))

    def message(w, slot, side):
        planes = pl.ds(depth - 2, 2) if side == 0 else pl.ds(0, 2)
        return remote(
            vel.at[0, w, :, planes, body, :],
            vel_msg.at[slot, side, w, :, :, body, :],
            msg_send.at[slot, side, w],
            msg_recv.at[slot, side, w],
            gz=here + 1 if side == 0 else here - 1,
        )

    def middle(w, cycle, side):
        return remote(
            vel.at[1, w, :, depth - 2 if side == 0 else 1, body, :],
            vel_mid.at[cycle, side, w, :, body, :],
            mid_send.at[cycle, side, w],
            mid_recv.at[cycle, side, w],
            gz=here + 1 if side == 0 else here - 1,
        )

    goes = (has_down, has_up)
    comes = (has_up, has_down)

    for copy in small:
        copy.wait()
    source_row = (source_depth[0] - here * depth + 1) * rows + source_column[0] // cols
    source_col = source_column[0] % cols
    for z in range(depth + 3):
        hit = (row + z * rows == source_row) & (lane == source_col)
        source_at[z] = jnp.where(hit, time_step, 0.0)
    cells = (depth + 2) * rows
    receiver_row = (receiver_depth[...] - here * depth + 1) * rows + receiver_column[...] // cols
    receiver_col = receiver_column[...] % cols
    twice_row = jnp.concatenate([receiver_row, receiver_row], axis=1)
    twice_col = jnp.concatenate([receiver_col, receiver_col], axis=1)
    in_row = lax.broadcasted_iota(jnp.int32, (cells, 2 * receivers), 0) == twice_row
    in_col = lax.broadcasted_iota(jnp.int32, (cols, 2 * receivers), 0) == twice_col
    in_col = jnp.where(in_col, 1.0, 0.0).astype(jnp.bfloat16)
    in_col = jnp.concatenate([in_col, in_col], axis=1)

    def in_bf16(f):
        return f.astype(jnp.bfloat16).astype(jnp.float32)

    amounts = time_step * traces[0]
    high = in_bf16(amounts)
    middle_part = in_bf16(amounts - high)
    low = in_bf16((amounts - high) - middle_part)
    parts[0] = jnp.concatenate([high, middle_part], axis=1)
    parts[1] = jnp.concatenate([low, jnp.zeros_like(low)], axis=1)

    def receivers_at(n, carry):
        spread = [
            jnp.where(in_row, parts[i, pl.ds(n, 1), :], 0.0).astype(jnp.bfloat16) for i in range(2)
        ]
        inject[n] = lax.dot_general(
            jnp.concatenate(spread, axis=1),
            in_col,
            (((1,), (1,)), ((), ())),
            preferred_element_type=jnp.float32,
        ).reshape(depth + 2, rows, cols)
        return carry

    lax.fori_loop(0, steps, receivers_at, 0)
    image[...] = jnp.zeros_like(image)

    for copy in loads[1:]:
        copy.wait()
    mat[...] = time_step * mat[...]

    def v(parity, slot, w, c, e, at=body):
        if 0 <= e < depth:
            return vel[parity, w, c, e, at, :]
        side = 0 if e < 0 else 1
        if parity == 0:
            return vel_msg[slot, side, w, c, e + 2 if e < 0 else e - depth, at, :]
        if e in (-1, depth):
            return vel_near[side, w, c, at, :]
        return vel_mid[slot, side, w, c, at, :]

    def s_at(w, f, e):
        if 0 <= e < depth:
            return sig, (w, f, e), True
        if e in (-1, depth):
            return sig_near, (0 if e < 0 else 1, w, f), True
        return sig_far, (w, {SXZ: 0, SYZ: 1, SZZ: 2}[f]), False

    def s(w, f, e, at=body):
        ref, index, guarded = s_at(w, f, e)
        return ref[(*index, at if guarded else whole, slice(None))]

    def add_s(w, f, e, change):
        ref, index, guarded = s_at(w, f, e)
        value = ref[(*index, body if guarded else whole, slice(None))] + change
        ref[(*index, body if guarded else whole, slice(None))] = value
        return value

    def m(which, e):
        if 0 <= e < depth:
            return mat[which, e]
        if e in (-1, depth):
            return mat_near[0 if e < 0 else 1, which]
        return mat_far[0 if e < 0 else which]

    def velocity(w, e, n, old, slot, parts_of=(0, 1, 2)):
        sxz, syz = s(w, SXZ, e), s(w, SYZ, e)
        if 0 in parts_of or 1 in parts_of:
            sxx, syy, sxy = s(w, SXX, e), s(w, SYY, e), s(w, SXY, e)
        forces = {}
        if 0 in parts_of:
            forces[0] = (s(w, SXX, e, after) - sxx) + b_y(sxy) + (sxz - s(w, SXZ, e - 1))
        if 1 in parts_of:
            forces[1] = (sxy - s(w, SXY, e, before)) + f_y(syy) + (syz - s(w, SYZ, e - 1))
        if 2 in parts_of:
            up = s(w, SZZ, e + 1) - s(w, SZZ, e)
            forces[2] = (sxz - s(w, SXZ, e, before)) + b_y(syz) + up
        buoyancy = m(0, e)
        for c, force in forces.items():
            moved = v(old, slot, w, c, e) + buoyancy * force
            if c == 2 and w == 1:
                moved = moved + inject[n, e + 1]
            if 0 <= e < depth:
                vel[1 - old, w, c, e, body, :] = moved
            else:
                vel_near[0 if e < 0 else 1, w, c, body, :] = moved

    def normal(parity, slot, w, e, n, spun=None, z_only=False):
        vx, vy, vz = [v(parity, slot, w, c, e) for c in range(3)]
        ex = vx - v(parity, slot, w, 0, e, before)
        ey = b_y(vy)
        ez = vz - v(parity, slot, w, 2, e - 1)
        common = m(1, e) * (ex + ey + ez)
        twice = 2.0 * m(2, e)
        if w == 0:
            common = common + source_at[e + 1] * wavelet[0, n]
        szz = add_s(w, SZZ, e, common + twice * ez)
        if z_only:
            return
        sxx = add_s(w, SXX, e, common + twice * ex)
        syy = add_s(w, SYY, e, common + twice * ey)
        if not 0 <= e < depth:
            return
        pressure = (sxx + syy + szz) * (1.0 / 3.0)
        if w == 0:
            press[parity, e] = pressure
        else:
            image[0, e] = image[0, e] + press[parity, e] * pressure
            if spun is not None:
                image[1, e] = image[1, e] + press[parity, e] * spin[spun]

    def shear(parity, slot, w, e, spun=None):
        vx, vy, vz = [v(parity, slot, w, c, e) for c in range(3)]
        x_up = v(parity, slot, w, 0, e + 1) - vx
        y_up = v(parity, slot, w, 1, e + 1) - vy
        z_along_x = v(parity, slot, w, 2, e, after) - vz
        z_along_y = f_y(vz)
        x_along_y = f_y(vx)
        y_along_x = v(parity, slot, w, 1, e, after) - vy
        mu = m(2, e)
        add_s(w, SXY, e, mu * (x_along_y + y_along_x))
        add_s(w, SXZ, e, mu * (x_up + z_along_x))
        add_s(w, SYZ, e, mu * (y_up + z_along_y))
        if w == 1:
            rotation = (z_along_y - y_up) + (x_up - z_along_x) + (y_along_x - x_along_y)
            if spun is None:
                image[1, e] = image[1, e] + press[parity, e] * rotation
            else:
                spin[spun] = rotation

    def shear_flat(parity, slot, w, e):
        x_along_y = f_y(v(parity, slot, w, 0, e))
        y_along_x = v(parity, slot, w, 1, e, after) - v(parity, slot, w, 1, e)
        add_s(w, SXY, e, m(2, e) * (x_along_y + y_along_x))

    def shear_deep(parity, slot, w, e):
        vx, vy, vz = [v(parity, slot, w, c, e) for c in range(3)]
        mu = m(2, e)
        z_along_x = v(parity, slot, w, 2, e, after) - vz
        add_s(w, SXZ, e, mu * ((v(parity, slot, w, 0, e + 1) - vx) + z_along_x))
        add_s(w, SYZ, e, mu * ((v(parity, slot, w, 1, e + 1) - vy) + f_y(vz)))

    def send_middle(cycle):
        for w in range(2):
            for side in range(2):
                up_to(goes[side], middle(w, cycle, side).start)

    def inside(cycle, n, send):
        for w in range(2):
            for e in range(1, depth):
                normal(0, None, w, e, n)
            shear(0, None, w, 0, spun=0)
            for e in range(1, last):
                shear(0, None, w, e)
            for e in (1, 2):
                velocity(w, e, n + 1, 0, None)
            normal(1, None, w, 2, n + 1)
            shear(1, None, w, 1, spun=1)
        up_to(send, lambda: send_middle(cycle))

    def lower(slot, w, n, final):
        up_to(goes[0], message(w, slot, 0).wait_send)
        up_to(comes[1], message(w, slot, 1).wait_recv)
        shear(0, slot, w, last)
        normal(0, slot, w, depth, n)
        shear_flat(0, slot, w, depth)
        shear_deep(0, slot, w, depth)
        if not final:
            normal(0, slot, w, depth + 1, n, z_only=True)
        velocity(w, last, n + 1, 0, slot)
        velocity(w, depth, n + 1, 0, slot, (0, 1) if final else (0, 1, 2))
        normal(1, slot, w, last, n + 1)
        shear(1, slot, w, last - 1)
        shear(1, slot, w, last)
        if final:
            return
        normal(1, slot, w, depth, n + 1)
        velocity(w, last, n + 2, 1, slot)
        velocity(w, last - 1, n + 2, 1, slot)
        up_to(goes[0], message(w, 1 - slot, 0).start)
        shear_flat(1, slot, w, depth)

    def upper(slot, n, final):
        for w in range(2):
            up_to(goes[1], message(w, slot, 1).wait_send)
            up_to(comes[0], message(w, slot, 0).wait_recv)
        for w in range(2):
            normal(0, slot, w, 0, n, spun=0)
            shear_deep(0, slot, w, -1)
            normal(0, slot, w, -1, n, z_only=final)
            if not final:
                shear_flat(0, slot, w, -1)
                shear_deep(0, slot, w, -2)
            velocity(w, 0, n + 1, 0, slot)
            velocity(w, -1, n + 1, 0, slot, (2,) if final else (0, 1, 2))
            normal(1, slot, w, 0, n + 1)
            normal(1, slot, w, 1, n + 1, spun=1)
            shear(1, slot, w, 0)
            if not final:
                shear_deep(1, slot, w, -1)
                velocity(w, 0, n + 2, 1, slot)
                velocity(w, 1, n + 2, 1, slot)
        if final:
            return
        for w in range(2):
            up_to(goes[1], message(w, 1 - slot, 1).start)
        for w in range(2):
            shear_flat(1, slot, w, -1)

    def catch_up(cycle, n):
        for w in range(2):
            for side in range(2):
                up_to(comes[side], middle(w, cycle, side).wait_recv)
        for w in range(2):
            shear_deep(1, cycle, w, depth)
            normal(1, cycle, w, depth + 1, n, z_only=True)
            normal(1, cycle, w, -1, n)
            shear_deep(1, cycle, w, -2)

    up_to(comes[1], first_up[0].wait_recv)
    for w in range(2):
        velocity(w, last, 0, 1, None)
        velocity(w, last - 1, 0, 1, None)
        up_to(goes[0], message(w, 0, 0).start)
    for w in range(2):
        velocity(w, 1, 0, 1, None)
        velocity(w, 0, 0, 1, None, (2,))
        for e in range(1, depth):
            normal(0, None, w, e, 0)
        for e in range(1, last):
            shear(0, None, w, e)
        velocity(w, 2, 1, 0, None)
        velocity(w, 1, 1, 0, None, (2,))
        normal(1, None, w, 2, 1)
    up_to(comes[0], first_down[0].wait_recv)
    for w in range(2):
        velocity(w, 0, 0, 1, None, (0, 1))
    for w in range(2):
        up_to(goes[1], message(w, 0, 1).start)
    for w in range(2):
        shear(0, None, w, 0, spun=0)
        velocity(w, 1, 1, 0, None, (0, 1))
        shear(1, None, w, 1, spun=1)
    send_middle(0)
    up_to(comes[1], lambda: [copy.wait_recv() for copy in first_up[1:]])
    up_to(comes[0], lambda: [copy.wait_recv() for copy in first_down[1:]])
    mat_near[...] = time_step * mat_near[...]
    mat_far[...] = time_step * mat_far[...]

    up_to(has_down, first_down[0].wait_send)
    up_to(has_up, first_up[0].wait_send)

    cycles = steps // 2

    def cycle_body(cycle, carry):
        slot = lax.rem(cycle, 2)
        n = 2 * cycle
        for w in range(2):
            lower(slot, w, n, False)
        upper(slot, n, False)
        for w in range(2):
            for side in range(2):
                up_to(goes[side], middle(w, cycle, side).wait_send)
        inside(cycle + 1, n + 2, cycle < cycles - 2)
        catch_up(cycle, n + 1)
        return carry

    lax.fori_loop(0, cycles - 1, cycle_body, 0)

    def to_shot(half, hop, source):
        planes = pl.ds(2 * half, 2)
        return remote(
            image.at[:, planes],
            out.at[source, :, planes],
            sum_send.at[half, hop],
            sum_recv.at[half, hop],
            shot=lax.rem(shot + hop, shots),
        )

    def keep(half):
        planes = pl.ds(2 * half, 2)
        return pltpu.make_async_copy(image.at[:, planes], out.at[shot, :, planes], keep_sem.at[half])

    def hand_over(half):
        for hop in (2, 1, 3):
            to_shot(half, hop, shot).start()
        keep(half).start()

    end = (cycles - 1) % 2
    for w in range(2):
        lower(end, w, steps - 2, True)
    hand_over(1)
    upper(end, steps - 2, True)
    hand_over(0)
    up_to(has_down, lambda: [copy.wait_send() for copy in first_down[1:]])
    up_to(has_up, lambda: [copy.wait_send() for copy in first_up[1:]])
    for half in (1, 0):
        keep(half).wait()
        for hop in others:
            to_shot(half, hop, lax.rem(shot + shots - hop, shots)).wait_recv()
    for half in (1, 0):
        for hop in others:
            to_shot(half, hop, shot).wait_send()


def solution(mesh):
    slabs, shots = mesh.shape["gz"], mesh.shape["shot"]

    def on_device(wavefields, earth, s_depth, s_column, wavelet, r_depth, r_column, traces):
        depth, rows, cols = earth.shape[1:]
        steps, receivers = traces.shape[1:]
        assert depth == 4 and shots == 4 and steps % 2 == 0 and steps >= 4
        dims = (slabs, shots, depth, rows, cols, steps, receivers)
        padded = rows + 2 * GUARD
        f32 = jnp.float32
        mids = steps // 2 - 1
        hbm = pl.BlockSpec(memory_space=pltpu.HBM)
        dma = pltpu.SemaphoreType.DMA
        by_shot = pl.pallas_call(
            functools.partial(window_kernel, dims),
            out_shape=jax.ShapeDtypeStruct((shots, 2, depth, rows, cols), f32),
            in_specs=[hbm] * 8,
            out_specs=hbm,
            scratch_shapes=[
                pltpu.VMEM((2, 2, 3, depth, padded, cols), f32),
                pltpu.VMEM((2, 2, 2, 3, 2, padded, cols), f32),
                pltpu.VMEM((mids, 2, 2, 3, padded, cols), f32),
                pltpu.VMEM((2, 2, 3, padded, cols), f32),
                pltpu.VMEM((2, 6, depth, padded, cols), f32),
                pltpu.VMEM((2, 2, 6, padded, cols), f32),
                pltpu.VMEM((2, 3, rows, cols), f32),
                pltpu.VMEM((3, depth, rows, cols), f32),
                pltpu.VMEM((2, 3, rows, cols), f32),
                pltpu.VMEM((3, rows, cols), f32),
                pltpu.VMEM((depth + 3, rows, cols), f32),
                pltpu.VMEM((steps, depth + 2, rows, cols), f32),
                pltpu.VMEM((2, depth, rows, cols), f32),
                pltpu.VMEM((2, rows, cols), f32),
                pltpu.VMEM((2, depth, rows, cols), f32),
                pltpu.VMEM((2, steps, 2 * receivers), f32),
                pltpu.SMEM(s_depth.shape, jnp.int32),
                pltpu.SMEM(s_column.shape, jnp.int32),
                pltpu.SMEM(wavelet.shape, f32),
                pltpu.VMEM(r_depth.shape, jnp.int32),
                pltpu.VMEM(r_column.shape, jnp.int32),
                pltpu.VMEM(traces.shape, f32),
                dma((3,)),
                dma((6,)),
                dma((2,)),
                dma((2, 6)),
                dma((2, 6)),
                dma((2, 2, 2)),
                dma((2, 2, 2)),
                dma((mids, 2, 2)),
                dma((mids, 2, 2)),
                dma((2, shots)),
                dma((2, shots)),
            ],
            compiler_params=pltpu.CompilerParams(
                collective_id=0, has_side_effects=True
            ),
        )(wavefields[0], earth, s_depth, s_column, wavelet, r_depth, r_column, traces)
        return sum(by_shot[i] for i in range(1, shots)) / steps + by_shot[0] / steps

    sharded = P(("parts", "shot"))
    return jax.shard_map(
        on_device,
        mesh=mesh,
        in_specs=(
            P(("parts", "shot"), None, None, "gz", None, None),
            P("parts", "gz", None, None),
            sharded,
            sharded,
            P(("parts", "shot"), None),
            P(("parts", "shot"), None),
            P(("parts", "shot"), None),
            P(("parts", "shot"), None, None),
        ),
        out_specs=P("parts", "gz", None, None),
        check_vma=False,
    )
```

```python
import functools
import itertools

import jax
import jax.numpy as jnp
from jax import lax
from jax.experimental import pallas as pl
from jax.experimental.pallas import tpu as pltpu
from jax.sharding import PartitionSpec as P

MESH = pl.DeviceIdType.MESH
time_step = 0.15
GUARD = 8
SXX, SYY, SZZ, SXY, SXZ, SYZ = range(6)


def window_kernel(
    dims,
    fields_in,
    earth_in,
    source_depth_in,
    source_column_in,
    wavelet_in,
    receiver_depth_in,
    receiver_column_in,
    traces_in,
    out,
    vel,
    vel_msg,
    vel_mid,
    vel_near,
    sig,
    sig_near,
    sig_far,
    mat,
    mat_near,
    mat_far,
    source_at,
    inject,
    press,
    spin,
    image,
    parts,
    source_depth,
    source_column,
    wavelet,
    receiver_depth,
    receiver_column,
    traces,
    load_sem,
    small_sem,
    keep_sem,
    near_sem,
    peers_sem,
    ready_sem,
    first_send,
    first_recv,
    msg_send,
    msg_recv,
    mid_send,
    mid_recv,
    sum_send,
    sum_recv,
):
    slabs, shots, depth, rows, cols, steps, receivers = dims
    here = lax.axis_index("gz")
    shot = lax.axis_index("shot")
    has_up, has_down = here > 0, here < slabs - 1
    last = depth - 1
    whole = pl.ds(0, rows)
    body = pl.ds(GUARD, rows)
    after = pl.ds(GUARD + 1, rows)
    before = pl.ds(GUARD - 1, rows)
    lane = lax.broadcasted_iota(jnp.int32, (rows, cols), 1)
    row = lax.broadcasted_iota(jnp.int32, (rows, cols), 0)
    at_first, at_last = lane == 0, lane == cols - 1

    def b_y(f):
        return f - jnp.where(at_first, 0.0, pltpu.roll(f, 1, 1))

    def f_y(f):
        return jnp.where(at_last, 0.0, pltpu.roll(f, cols - 1, 1)) - f

    loads = [
        pltpu.make_async_copy(
            fields_in.at[:, 3:9], sig.at[:, :, :, body, :], load_sem.at[0]
        ),
        pltpu.make_async_copy(
            fields_in.at[:, 0:3], vel.at[1, :, :, :, body, :], load_sem.at[1]
        ),
        pltpu.make_async_copy(earth_in, mat, load_sem.at[2]),
    ]
    small = [
        pltpu.make_async_copy(src, dst, small_sem.at[i])
        for i, (src, dst) in enumerate(
            (
                (source_depth_in, source_depth),
                (source_column_in, source_column),
                (wavelet_in, wavelet),
                (receiver_depth_in, receiver_depth),
                (receiver_column_in, receiver_column),
                (traces_in, traces),
            )
        )
    ]
    for copy in loads + small:
        copy.start()

    barrier = pltpu.get_barrier_semaphore()

    def up_to(where, then):
        @pl.when(where)
        def _():
            then()

    def greet(**to):
        pl.semaphore_signal(barrier, inc=1, device_id=to, device_id_type=MESH)

    others = range(1, shots)
    odd = lax.rem(here, 2) == 1
    even = lax.rem(here, 2) == 0

    def greet_all():
        greet(gz=here - 1)
        up_to(has_down, lambda: greet(gz=here + 1))
        for hop in others:
            greet(shot=lax.rem(shot + hop, shots))

    def answer(side, **to):
        pl.semaphore_signal(near_sem.at[side], inc=1, device_id=to, device_id_type=MESH)

    up_to(odd, greet_all)
    beside = jnp.where(has_up, 1, 0) + jnp.where(has_down, 1, 0)
    pl.semaphore_wait(barrier, jnp.where(even, beside, shots - 1))
    up_to(even & has_down, lambda: answer(0, gz=here + 1))
    up_to(even & has_up, lambda: answer(1, gz=here - 1))

    def remote(src, dst, send, recv, **to):
        return pltpu.make_async_remote_copy(
            src_ref=src, dst_ref=dst, send_sem=send, recv_sem=recv, device_id=to, device_id_type=MESH
        )

    downs = (
        (sig.at[:, 4:6, last, body, :], sig_near.at[0, :, 4:6, body, :]),
        (fields_in.at[:, 3:7, last], sig_near.at[0, :, 0:4, body, :]),
        (fields_in.at[:, 7:9, last - 1], sig_far.at[:, 0:2]),
        (earth_in.at[:, last], mat_near.at[0]),
        (earth_in.at[2, last - 1], mat_far.at[0]),
    )
    ups = (
        (sig.at[:, 2:3, 0, body, :], sig_near.at[1, :, 2:3, body, :]),
        (fields_in.at[:, 3:5, 0], sig_near.at[1, :, 0:2, body, :]),
        (fields_in.at[:, 6:9, 0], sig_near.at[1, :, 3:6, body, :]),
        (fields_in.at[:, 5, 1], sig_far.at[:, 2]),
        (earth_in.at[:, 0], mat_near.at[1]),
        (earth_in.at[1:3, 1], mat_far.at[1:3]),
    )
    first_down = [
        remote(src, dst, first_send.at[0, i], first_recv.at[0, i], gz=here + 1)
        for i, (src, dst) in enumerate(downs)
    ]
    first_up = [
        remote(src, dst, first_send.at[1, i], first_recv.at[1, i], gz=here - 1)
        for i, (src, dst) in enumerate(ups)
    ]
    loads[0].wait()
    up_to(odd & has_down, lambda: pl.semaphore_wait(near_sem.at[1], 1))
    up_to(has_down, first_down[0].start)
    up_to(even & has_up, first_up[0].start)
    up_to(has_down, lambda: [copy.start() for copy in first_down[1:]])
    up_to(even & has_up, lambda: [copy.start() for copy in first_up[1:]])

    zeros = jnp.zeros((GUARD, cols), jnp.float32)

    def clear_around(ref, *extents):
        for index in itertools.product(*[range(extent) for extent in extents]):
            ref[(*index, pl.ds(0, GUARD), slice(None))] = zeros
            ref[(*index, pl.ds(GUARD + rows, GUARD), slice(None))] = zeros

    clear_around(sig, 2, 6, depth)
    clear_around(vel, 2, 2, 3, depth)
    clear_around(vel_near, 2, 2, 3)
    clear_around(vel_msg, 2, 2, 2, 3, 2)
    clear_around(vel_mid, steps // 2 - 1, 2, 2, 3)
    clear_around(sig_near, 2, 2, 6)

    def outside(side):
        far = pl.ds(0, 2) if side == 0 else pl.ds(2, 1)
        for view in (
            vel_msg.at[:, side, :, :, :, body, :],
            vel_mid.at[:, side, :, :, body, :],
            sig_near.at[side, :, :, body, :],
            sig_far.at[:, far],
            mat_near.at[side],
            mat_far.at[pl.ds(side, 1 + side)],
        ):
            view[...] = jnp.zeros(view.shape, jnp.float32)

    up_to(here == 0, lambda: outside(0))
    up_to(here == slabs - 1, lambda: outside(1))

    def message(w, slot, side):
        planes = pl.ds(depth - 2, 2) if side == 0 else pl.ds(0, 2)
        return remote(
            vel.at[0, w, :, planes, body, :],
            vel_msg.at[slot, side, w, :, :, body, :],
            msg_send.at[slot, side, w],
            msg_recv.at[slot, side, w],
            gz=here + 1 if side == 0 else here - 1,
        )

    def middle(w, cycle, side):
        return remote(
            vel.at[1, w, :, depth - 2 if side == 0 else 1, body, :],
            vel_mid.at[cycle, side, w, :, body, :],
            mid_send.at[cycle, side, w],
            mid_recv.at[cycle, side, w],
            gz=here + 1 if side == 0 else here - 1,
        )

    goes = (has_down, has_up)
    comes = (has_up, has_down)

    for copy in small:
        copy.wait()
    source_row = (source_depth[0] - here * depth + 1) * rows + source_column[0] // cols
    source_col = source_column[0] % cols
    for z in range(depth + 3):
        hit = (row + z * rows == source_row) & (lane == source_col)
        source_at[z] = jnp.where(hit, time_step, 0.0)
    cells = (depth + 2) * rows
    receiver_row = (receiver_depth[...] - here * depth + 1) * rows + receiver_column[...] // cols
    receiver_col = receiver_column[...] % cols
    twice_row = jnp.concatenate([receiver_row, receiver_row], axis=1)
    twice_col = jnp.concatenate([receiver_col, receiver_col], axis=1)
    in_row = lax.broadcasted_iota(jnp.int32, (cells, 2 * receivers), 0) == twice_row
    in_col = lax.broadcasted_iota(jnp.int32, (cols, 2 * receivers), 0) == twice_col
    in_col = jnp.where(in_col, 1.0, 0.0).astype(jnp.bfloat16)
    in_col = jnp.concatenate([in_col, in_col], axis=1)

    def in_bf16(f):
        return f.astype(jnp.bfloat16).astype(jnp.float32)

    amounts = time_step * traces[0]
    high = in_bf16(amounts)
    middle_part = in_bf16(amounts - high)
    low = in_bf16((amounts - high) - middle_part)
    parts[0] = jnp.concatenate([high, middle_part], axis=1)
    parts[1] = jnp.concatenate([low, jnp.zeros_like(low)], axis=1)

    def receivers_at(n, carry):
        spread = [
            jnp.where(in_row, parts[i, pl.ds(n, 1), :], 0.0).astype(jnp.bfloat16) for i in range(2)
        ]
        inject[n] = lax.dot_general(
            jnp.concatenate(spread, axis=1),
            in_col,
            (((1,), (1,)), ((), ())),
            preferred_element_type=jnp.float32,
        ).reshape(depth + 2, rows, cols)
        return carry

    lax.fori_loop(0, steps, receivers_at, 0)
    image[...] = jnp.zeros_like(image)

    for copy in loads[1:]:
        copy.wait()
    mat[...] = time_step * mat[...]

    def v(parity, slot, w, c, e, at=body):
        if 0 <= e < depth:
            return vel[parity, w, c, e, at, :]
        side = 0 if e < 0 else 1
        if parity == 0:
            return vel_msg[slot, side, w, c, e + 2 if e < 0 else e - depth, at, :]
        if e in (-1, depth):
            return vel_near[side, w, c, at, :]
        return vel_mid[slot, side, w, c, at, :]

    def s_at(w, f, e):
        if 0 <= e < depth:
            return sig, (w, f, e), True
        if e in (-1, depth):
            return sig_near, (0 if e < 0 else 1, w, f), True
        return sig_far, (w, {SXZ: 0, SYZ: 1, SZZ: 2}[f]), False

    def s(w, f, e, at=body):
        ref, index, guarded = s_at(w, f, e)
        return ref[(*index, at if guarded else whole, slice(None))]

    def add_s(w, f, e, change):
        ref, index, guarded = s_at(w, f, e)
        value = ref[(*index, body if guarded else whole, slice(None))] + change
        ref[(*index, body if guarded else whole, slice(None))] = value
        return value

    def m(which, e):
        if 0 <= e < depth:
            return mat[which, e]
        if e in (-1, depth):
            return mat_near[0 if e < 0 else 1, which]
        return mat_far[0 if e < 0 else which]

    def velocity(w, e, n, old, slot, parts_of=(0, 1, 2)):
        sxz, syz = s(w, SXZ, e), s(w, SYZ, e)
        if 0 in parts_of or 1 in parts_of:
            sxx, syy, sxy = s(w, SXX, e), s(w, SYY, e), s(w, SXY, e)
        forces = {}
        if 0 in parts_of:
            forces[0] = (s(w, SXX, e, after) - sxx) + b_y(sxy) + (sxz - s(w, SXZ, e - 1))
        if 1 in parts_of:
            forces[1] = (sxy - s(w, SXY, e, before)) + f_y(syy) + (syz - s(w, SYZ, e - 1))
        if 2 in parts_of:
            up = s(w, SZZ, e + 1) - s(w, SZZ, e)
            forces[2] = (sxz - s(w, SXZ, e, before)) + b_y(syz) + up
        buoyancy = m(0, e)
        for c, force in forces.items():
            moved = v(old, slot, w, c, e) + buoyancy * force
            if c == 2 and w == 1:
                moved = moved + inject[n, e + 1]
            if 0 <= e < depth:
                vel[1 - old, w, c, e, body, :] = moved
            else:
                vel_near[0 if e < 0 else 1, w, c, body, :] = moved

    def normal(parity, slot, w, e, n, spun=None, z_only=False):
        vx, vy, vz = [v(parity, slot, w, c, e) for c in range(3)]
        ex = vx - v(parity, slot, w, 0, e, before)
        ey = b_y(vy)
        ez = vz - v(parity, slot, w, 2, e - 1)
        common = m(1, e) * (ex + ey + ez)
        twice = 2.0 * m(2, e)
        if w == 0:
            common = common + source_at[e + 1] * wavelet[0, n]
        szz = add_s(w, SZZ, e, common + twice * ez)
        if z_only:
            return
        sxx = add_s(w, SXX, e, common + twice * ex)
        syy = add_s(w, SYY, e, common + twice * ey)
        if not 0 <= e < depth:
            return
        pressure = (sxx + syy + szz) * (1.0 / 3.0)
        if w == 0:
            press[parity, e] = pressure
        else:
            image[0, e] = image[0, e] + press[parity, e] * pressure
            if spun is not None:
                image[1, e] = image[1, e] + press[parity, e] * spin[spun]

    def shear(parity, slot, w, e, spun=None):
        vx, vy, vz = [v(parity, slot, w, c, e) for c in range(3)]
        x_up = v(parity, slot, w, 0, e + 1) - vx
        y_up = v(parity, slot, w, 1, e + 1) - vy
        z_along_x = v(parity, slot, w, 2, e, after) - vz
        z_along_y = f_y(vz)
        x_along_y = f_y(vx)
        y_along_x = v(parity, slot, w, 1, e, after) - vy
        mu = m(2, e)
        add_s(w, SXY, e, mu * (x_along_y + y_along_x))
        add_s(w, SXZ, e, mu * (x_up + z_along_x))
        add_s(w, SYZ, e, mu * (y_up + z_along_y))
        if w == 1:
            rotation = (z_along_y - y_up) + (x_up - z_along_x) + (y_along_x - x_along_y)
            if spun is None:
                image[1, e] = image[1, e] + press[parity, e] * rotation
            else:
                spin[spun] = rotation

    def shear_flat(parity, slot, w, e):
        x_along_y = f_y(v(parity, slot, w, 0, e))
        y_along_x = v(parity, slot, w, 1, e, after) - v(parity, slot, w, 1, e)
        add_s(w, SXY, e, m(2, e) * (x_along_y + y_along_x))

    def shear_deep(parity, slot, w, e):
        vx, vy, vz = [v(parity, slot, w, c, e) for c in range(3)]
        mu = m(2, e)
        z_along_x = v(parity, slot, w, 2, e, after) - vz
        add_s(w, SXZ, e, mu * ((v(parity, slot, w, 0, e + 1) - vx) + z_along_x))
        add_s(w, SYZ, e, mu * ((v(parity, slot, w, 1, e + 1) - vy) + f_y(vz)))

    def send_middle(cycle):
        for w in range(2):
            for side in range(2):
                up_to(goes[side], middle(w, cycle, side).start)

    def inside(cycle, n, send):
        for w in range(2):
            for e in range(1, depth):
                normal(0, None, w, e, n)
            shear(0, None, w, 0, spun=0)
            for e in range(1, last):
                shear(0, None, w, e)
            for e in (1, 2):
                velocity(w, e, n + 1, 0, None)
            normal(1, None, w, 2, n + 1)
            shear(1, None, w, 1, spun=1)
        up_to(send, lambda: send_middle(cycle))

    def lower(slot, w, n, final):
        up_to(goes[0], message(w, slot, 0).wait_send)
        up_to(comes[1], message(w, slot, 1).wait_recv)
        shear(0, slot, w, last)
        normal(0, slot, w, depth, n)
        shear_flat(0, slot, w, depth)
        shear_deep(0, slot, w, depth)
        if not final:
            normal(0, slot, w, depth + 1, n, z_only=True)
        velocity(w, last, n + 1, 0, slot)
        velocity(w, depth, n + 1, 0, slot, (0, 1) if final else (0, 1, 2))
        normal(1, slot, w, last, n + 1)
        shear(1, slot, w, last - 1)
        shear(1, slot, w, last)
        if final:
            return
        normal(1, slot, w, depth, n + 1)
        velocity(w, last, n + 2, 1, slot)
        velocity(w, last - 1, n + 2, 1, slot)
        up_to(goes[0], message(w, 1 - slot, 0).start)
        shear_flat(1, slot, w, depth)

    def upper(slot, w, n, final):
        up_to(comes[0], message(w, slot, 0).wait_recv)
        normal(0, slot, w, 0, n, spun=0)
        shear_deep(0, slot, w, -1)
        normal(0, slot, w, -1, n, z_only=final)
        if not final:
            shear_flat(0, slot, w, -1)
            shear_deep(0, slot, w, -2)
        velocity(w, 0, n + 1, 0, slot)
        velocity(w, -1, n + 1, 0, slot, (2,) if final else (0, 1, 2))
        normal(1, slot, w, 0, n + 1)
        normal(1, slot, w, 1, n + 1, spun=1)
        shear(1, slot, w, 0)
        up_to(goes[1], message(w, slot, 1).wait_send)
        if final:
            return
        shear_deep(1, slot, w, -1)
        velocity(w, 0, n + 2, 1, slot)
        velocity(w, 1, n + 2, 1, slot)
        up_to(goes[1], message(w, 1 - slot, 1).start)
        shear_flat(1, slot, w, -1)

    def catch_up(cycle, n):
        for w in range(2):
            for side in range(2):
                up_to(comes[side], middle(w, cycle, side).wait_recv)
        for w in range(2):
            shear_deep(1, cycle, w, depth)
            normal(1, cycle, w, depth + 1, n, z_only=True)
            normal(1, cycle, w, -1, n)
            shear_deep(1, cycle, w, -2)

    up_to(comes[1], first_up[0].wait_recv)
    for w in range(2):
        velocity(w, last, 0, 1, None)
        velocity(w, last - 1, 0, 1, None)
        up_to(goes[0], message(w, 0, 0).start)
    for w in range(2):
        velocity(w, 1, 0, 1, None)
        velocity(w, 0, 0, 1, None, (2,))
        for e in range(1, depth):
            normal(0, None, w, e, 0)
        for e in range(1, last):
            shear(0, None, w, e)
        velocity(w, 2, 1, 0, None)
        velocity(w, 1, 1, 0, None, (2,))
        normal(1, None, w, 2, 1)

    def upper_side_is_there():
        pl.semaphore_wait(near_sem.at[0], 1)
        for copy in first_up:
            copy.start()
        for hop in others:
            to = {"shot": lax.rem(shot + hop, shots)}
            pl.semaphore_signal(peers_sem, inc=1, device_id=to, device_id_type=MESH)

    up_to(odd, upper_side_is_there)
    up_to(comes[0], first_down[0].wait_recv)
    for w in range(2):
        velocity(w, 0, 0, 1, None, (0, 1))
    for w in range(2):
        up_to(goes[1], message(w, 0, 1).start)
    for w in range(2):
        shear(0, None, w, 0, spun=0)
        velocity(w, 1, 1, 0, None, (0, 1))
        shear(1, None, w, 1, spun=1)
    send_middle(0)
    up_to(comes[1], lambda: [copy.wait_recv() for copy in first_up[1:]])
    up_to(comes[0], lambda: [copy.wait_recv() for copy in first_down[1:]])
    mat_near[...] = time_step * mat_near[...]
    mat_far[...] = time_step * mat_far[...]

    up_to(has_down, first_down[0].wait_send)
    up_to(has_up, first_up[0].wait_send)

    cycles = steps // 2

    def cycle_body(cycle, carry):
        slot = lax.rem(cycle, 2)
        n = 2 * cycle
        for w in range(2):
            lower(slot, w, n, False)
        for w in range(2):
            upper(slot, w, n, False)
        for w in range(2):
            for side in range(2):
                up_to(goes[side], middle(w, cycle, side).wait_send)
        inside(cycle + 1, n + 2, cycle < cycles - 2)
        catch_up(cycle, n + 1)
        return carry

    lax.fori_loop(0, cycles - 1, cycle_body, 0)

    def to_shot(half, hop, source):
        planes = pl.ds(2 * half, 2)
        return remote(
            image.at[:, planes],
            out.at[source, :, planes],
            sum_send.at[half, hop],
            sum_recv.at[half, hop],
            shot=lax.rem(shot + hop, shots),
        )

    def keep(half):
        planes = pl.ds(2 * half, 2)
        return pltpu.make_async_copy(image.at[:, planes], out.at[shot, :, planes], keep_sem.at[half])

    def hand_over(half):
        for hop in (2, 1, 3):
            to_shot(half, hop, shot).start()
        keep(half).start()

    def pass_on():
        pl.semaphore_wait(peers_sem, shots - 1)
        pl.semaphore_signal(ready_sem, inc=1, device_id={"gz": here - 1}, device_id_type=MESH)

    up_to(odd, pass_on)
    end = (cycles - 1) % 2
    for w in range(2):
        lower(end, w, steps - 2, True)
    up_to(even, lambda: pl.semaphore_wait(ready_sem, 1))
    hand_over(1)
    for w in range(2):
        upper(end, w, steps - 2, True)
    hand_over(0)
    up_to(has_down, lambda: [copy.wait_send() for copy in first_down[1:]])
    up_to(has_up, lambda: [copy.wait_send() for copy in first_up[1:]])
    for half in (1, 0):
        keep(half).wait()
        for hop in others:
            to_shot(half, hop, lax.rem(shot + shots - hop, shots)).wait_recv()
    for half in (1, 0):
        for hop in others:
            to_shot(half, hop, shot).wait_send()


def solution(mesh):
    slabs, shots = mesh.shape["gz"], mesh.shape["shot"]

    def on_device(wavefields, earth, s_depth, s_column, wavelet, r_depth, r_column, traces):
        depth, rows, cols = earth.shape[1:]
        steps, receivers = traces.shape[1:]
        assert depth == 4 and shots == 4 and slabs % 2 == 0 and steps % 2 == 0 and steps >= 4
        dims = (slabs, shots, depth, rows, cols, steps, receivers)
        padded = rows + 2 * GUARD
        f32 = jnp.float32
        mids = steps // 2 - 1
        hbm = pl.BlockSpec(memory_space=pltpu.HBM)
        dma = pltpu.SemaphoreType.DMA
        by_shot = pl.pallas_call(
            functools.partial(window_kernel, dims),
            out_shape=jax.ShapeDtypeStruct((shots, 2, depth, rows, cols), f32),
            in_specs=[hbm] * 8,
            out_specs=hbm,
            scratch_shapes=[
                pltpu.VMEM((2, 2, 3, depth, padded, cols), f32),
                pltpu.VMEM((2, 2, 2, 3, 2, padded, cols), f32),
                pltpu.VMEM((mids, 2, 2, 3, padded, cols), f32),
                pltpu.VMEM((2, 2, 3, padded, cols), f32),
                pltpu.VMEM((2, 6, depth, padded, cols), f32),
                pltpu.VMEM((2, 2, 6, padded, cols), f32),
                pltpu.VMEM((2, 3, rows, cols), f32),
                pltpu.VMEM((3, depth, rows, cols), f32),
                pltpu.VMEM((2, 3, rows, cols), f32),
                pltpu.VMEM((3, rows, cols), f32),
                pltpu.VMEM((depth + 3, rows, cols), f32),
                pltpu.VMEM((steps, depth + 2, rows, cols), f32),
                pltpu.VMEM((2, depth, rows, cols), f32),
                pltpu.VMEM((2, rows, cols), f32),
                pltpu.VMEM((2, depth, rows, cols), f32),
                pltpu.VMEM((2, steps, 2 * receivers), f32),
                pltpu.SMEM(s_depth.shape, jnp.int32),
                pltpu.SMEM(s_column.shape, jnp.int32),
                pltpu.SMEM(wavelet.shape, f32),
                pltpu.VMEM(r_depth.shape, jnp.int32),
                pltpu.VMEM(r_column.shape, jnp.int32),
                pltpu.VMEM(traces.shape, f32),
                dma((3,)),
                dma((6,)),
                dma((2,)),
                pltpu.SemaphoreType.REGULAR((2,)),
                pltpu.SemaphoreType.REGULAR,
                pltpu.SemaphoreType.REGULAR,
                dma((2, 6)),
                dma((2, 6)),
                dma((2, 2, 2)),
                dma((2, 2, 2)),
                dma((mids, 2, 2)),
                dma((mids, 2, 2)),
                dma((2, shots)),
                dma((2, shots)),
            ],
            compiler_params=pltpu.CompilerParams(
                collective_id=0, has_side_effects=True
            ),
        )(wavefields[0], earth, s_depth, s_column, wavelet, r_depth, r_column, traces)
        return sum(by_shot[i] for i in range(1, shots)) / steps + by_shot[0] / steps

    sharded = P(("parts", "shot"))
    return jax.shard_map(
        on_device,
        mesh=mesh,
        in_specs=(
            P(("parts", "shot"), None, None, "gz", None, None),
            P("parts", "gz", None, None),
            sharded,
            sharded,
            P(("parts", "shot"), None),
            P(("parts", "shot"), None),
            P(("parts", "shot"), None),
            P(("parts", "shot"), None, None),
        ),
        out_specs=P("parts", "gz", None, None),
        check_vma=False,
    )
```

```python
import functools
import itertools

import jax
import jax.numpy as jnp
from jax import lax
from jax.experimental import pallas as pl
from jax.experimental.pallas import tpu as pltpu
from jax.sharding import PartitionSpec as P

MESH = pl.DeviceIdType.MESH
time_step = 0.15
GUARD = 8
SXX, SYY, SZZ, SXY, SXZ, SYZ = range(6)


def window_kernel(
    dims,
    fields_in,
    earth_in,
    source_depth_in,
    source_column_in,
    wavelet_in,
    receiver_depth_in,
    receiver_column_in,
    traces_in,
    out,
    vel,
    vel_msg,
    vel_mid,
    vel_near,
    sig,
    sig_near,
    sig_far,
    mat,
    mat_near,
    mat_far,
    source_at,
    inject,
    press,
    spin,
    image,
    parts,
    source_depth,
    source_column,
    wavelet,
    receiver_depth,
    receiver_column,
    traces,
    load_sem,
    small_sem,
    keep_sem,
    near_sem,
    peers_sem,
    ready_sem,
    first_send,
    first_recv,
    msg_send,
    msg_recv,
    mid_send,
    mid_recv,
    sum_send,
    sum_recv,
):
    slabs, shots, depth, rows, cols, steps, receivers = dims
    here = lax.axis_index("gz")
    shot = lax.axis_index("shot")
    has_up, has_down = here > 0, here < slabs - 1
    last = depth - 1
    whole = pl.ds(0, rows)
    body = pl.ds(GUARD, rows)
    after = pl.ds(GUARD + 1, rows)
    before = pl.ds(GUARD - 1, rows)
    lane = lax.broadcasted_iota(jnp.int32, (rows, cols), 1)
    row = lax.broadcasted_iota(jnp.int32, (rows, cols), 0)
    at_first, at_last = lane == 0, lane == cols - 1

    def b_y(f):
        return f - jnp.where(at_first, 0.0, pltpu.roll(f, 1, 1))

    def f_y(f):
        return jnp.where(at_last, 0.0, pltpu.roll(f, cols - 1, 1)) - f

    loads = [
        pltpu.make_async_copy(
            fields_in.at[:, 3:9], sig.at[:, :, :, body, :], load_sem.at[0]
        ),
        pltpu.make_async_copy(
            fields_in.at[:, 0:3], vel.at[1, :, :, :, body, :], load_sem.at[1]
        ),
        pltpu.make_async_copy(earth_in, mat, load_sem.at[2]),
    ]
    small = [
        pltpu.make_async_copy(src, dst, small_sem.at[i])
        for i, (src, dst) in enumerate(
            (
                (source_depth_in, source_depth),
                (source_column_in, source_column),
                (wavelet_in, wavelet),
                (receiver_depth_in, receiver_depth),
                (receiver_column_in, receiver_column),
                (traces_in, traces),
            )
        )
    ]
    for copy in loads + small:
        copy.start()

    barrier = pltpu.get_barrier_semaphore()

    def up_to(where, then):
        @pl.when(where)
        def _():
            then()

    def greet(**to):
        pl.semaphore_signal(barrier, inc=1, device_id=to, device_id_type=MESH)

    others = range(1, shots)
    odd = lax.rem(here, 2) == 1
    even = lax.rem(here, 2) == 0

    def greet_all():
        greet(gz=here - 1)
        up_to(has_down, lambda: greet(gz=here + 1))
        for hop in others:
            greet(shot=lax.rem(shot + hop, shots))

    def answer(side, **to):
        pl.semaphore_signal(near_sem.at[side], inc=1, device_id=to, device_id_type=MESH)

    up_to(odd, greet_all)
    beside = jnp.where(has_up, 1, 0) + jnp.where(has_down, 1, 0)
    pl.semaphore_wait(barrier, jnp.where(even, beside, shots - 1))
    up_to(even & has_down, lambda: answer(0, gz=here + 1))
    up_to(even & has_up, lambda: answer(1, gz=here - 1))

    def remote(src, dst, send, recv, **to):
        return pltpu.make_async_remote_copy(
            src_ref=src, dst_ref=dst, send_sem=send, recv_sem=recv, device_id=to, device_id_type=MESH
        )

    downs = (
        (sig.at[:, 4:6, last, body, :], sig_near.at[0, :, 4:6, body, :]),
        (fields_in.at[:, 3:7, last], sig_near.at[0, :, 0:4, body, :]),
        (fields_in.at[:, 7:9, last - 1], sig_far.at[:, 0:2]),
        (earth_in.at[:, last], mat_near.at[0]),
        (earth_in.at[2, last - 1], mat_far.at[0]),
    )
    ups = (
        (sig.at[:, 2:3, 0, body, :], sig_near.at[1, :, 2:3, body, :]),
        (fields_in.at[:, 3:5, 0], sig_near.at[1, :, 0:2, body, :]),
        (fields_in.at[:, 6:9, 0], sig_near.at[1, :, 3:6, body, :]),
        (fields_in.at[:, 5, 1], sig_far.at[:, 2]),
        (earth_in.at[:, 0], mat_near.at[1]),
        (earth_in.at[1:3, 1], mat_far.at[1:3]),
    )
    first_down = [
        remote(src, dst, first_send.at[0, i], first_recv.at[0, i], gz=here + 1)
        for i, (src, dst) in enumerate(downs)
    ]
    first_up = [
        remote(src, dst, first_send.at[1, i], first_recv.at[1, i], gz=here - 1)
        for i, (src, dst) in enumerate(ups)
    ]
    loads[0].wait()
    up_to(odd & has_down, lambda: pl.semaphore_wait(near_sem.at[1], 1))
    up_to(has_down, first_down[0].start)
    up_to(even & has_up, first_up[0].start)
    up_to(has_down, lambda: [copy.start() for copy in first_down[1:]])
    up_to(even & has_up, lambda: [copy.start() for copy in first_up[1:]])

    zeros = jnp.zeros((GUARD, cols), jnp.float32)

    def clear_around(ref, *extents):
        for index in itertools.product(*[range(extent) for extent in extents]):
            ref[(*index, pl.ds(0, GUARD), slice(None))] = zeros
            ref[(*index, pl.ds(GUARD + rows, GUARD), slice(None))] = zeros

    clear_around(sig, 2, 6, depth)
    clear_around(vel, 2, 2, 3, depth)
    clear_around(vel_near, 2, 2, 3)
    clear_around(vel_msg, 2, 2, 2, 3, 2)
    clear_around(vel_mid, steps // 2 - 1, 2, 2, 3)
    clear_around(sig_near, 2, 2, 6)

    def outside(side):
        far = pl.ds(0, 2) if side == 0 else pl.ds(2, 1)
        for view in (
            vel_msg.at[:, side, :, :, :, body, :],
            vel_mid.at[:, side, :, :, body, :],
            sig_near.at[side, :, :, body, :],
            sig_far.at[:, far],
            mat_near.at[side],
            mat_far.at[pl.ds(side, 1 + side)],
        ):
            view[...] = jnp.zeros(view.shape, jnp.float32)

    up_to(here == 0, lambda: outside(0))
    up_to(here == slabs - 1, lambda: outside(1))

    def message(w, slot, side):
        planes = pl.ds(depth - 2, 2) if side == 0 else pl.ds(0, 2)
        return remote(
            vel.at[0, w, :, planes, body, :],
            vel_msg.at[slot, side, w, :, :, body, :],
            msg_send.at[slot, side, w],
            msg_recv.at[slot, side, w],
            gz=here + 1 if side == 0 else here - 1,
        )

    def middle(w, cycle, side):
        return remote(
            vel.at[1, w, :, depth - 2 if side == 0 else 1, body, :],
            vel_mid.at[cycle, side, w, :, body, :],
            mid_send.at[cycle, side, w],
            mid_recv.at[cycle, side, w],
            gz=here + 1 if side == 0 else here - 1,
        )

    goes = (has_down, has_up)
    comes = (has_up, has_down)

    for copy in small:
        copy.wait()
    source_row = (source_depth[0] - here * depth + 1) * rows + source_column[0] // cols
    source_col = source_column[0] % cols
    for z in range(depth + 3):
        hit = (row + z * rows == source_row) & (lane == source_col)
        source_at[z] = jnp.where(hit, time_step, 0.0)
    cells = (depth + 2) * rows
    receiver_row = (receiver_depth[...] - here * depth + 1) * rows + receiver_column[...] // cols
    receiver_col = receiver_column[...] % cols
    twice_row = jnp.concatenate([receiver_row, receiver_row], axis=1)
    twice_col = jnp.concatenate([receiver_col, receiver_col], axis=1)
    in_row = lax.broadcasted_iota(jnp.int32, (cells, 2 * receivers), 0) == twice_row
    in_col = lax.broadcasted_iota(jnp.int32, (cols, 2 * receivers), 0) == twice_col
    in_col = jnp.where(in_col, 1.0, 0.0).astype(jnp.bfloat16)
    in_col = jnp.concatenate([in_col, in_col], axis=1)

    def in_bf16(f):
        return f.astype(jnp.bfloat16).astype(jnp.float32)

    amounts = time_step * traces[0]
    high = in_bf16(amounts)
    middle_part = in_bf16(amounts - high)
    low = in_bf16((amounts - high) - middle_part)
    parts[0] = jnp.concatenate([high, middle_part], axis=1)
    parts[1] = jnp.concatenate([low, jnp.zeros_like(low)], axis=1)

    def receivers_at(n, carry):
        spread = [
            jnp.where(in_row, parts[i, pl.ds(n, 1), :], 0.0).astype(jnp.bfloat16) for i in range(2)
        ]
        inject[n] = lax.dot_general(
            jnp.concatenate(spread, axis=1),
            in_col,
            (((1,), (1,)), ((), ())),
            preferred_element_type=jnp.float32,
        ).reshape(depth + 2, rows, cols)
        return carry

    lax.fori_loop(0, steps, receivers_at, 0)
    image[...] = jnp.zeros_like(image)

    for copy in loads[1:]:
        copy.wait()
    mat[...] = time_step * mat[...]

    def v(parity, slot, w, c, e, at=body):
        if 0 <= e < depth:
            return vel[parity, w, c, e, at, :]
        side = 0 if e < 0 else 1
        if parity == 0:
            return vel_msg[slot, side, w, c, e + 2 if e < 0 else e - depth, at, :]
        if e in (-1, depth):
            return vel_near[side, w, c, at, :]
        return vel_mid[slot, side, w, c, at, :]

    def s_at(w, f, e):
        if 0 <= e < depth:
            return sig, (w, f, e), True
        if e in (-1, depth):
            return sig_near, (0 if e < 0 else 1, w, f), True
        return sig_far, (w, {SXZ: 0, SYZ: 1, SZZ: 2}[f]), False

    def s(w, f, e, at=body):
        ref, index, guarded = s_at(w, f, e)
        return ref[(*index, at if guarded else whole, slice(None))]

    def add_s(w, f, e, change):
        ref, index, guarded = s_at(w, f, e)
        value = ref[(*index, body if guarded else whole, slice(None))] + change
        ref[(*index, body if guarded else whole, slice(None))] = value
        return value

    def m(which, e):
        if 0 <= e < depth:
            return mat[which, e]
        if e in (-1, depth):
            return mat_near[0 if e < 0 else 1, which]
        return mat_far[0 if e < 0 else which]

    def velocity(w, e, n, old, slot, parts_of=(0, 1, 2)):
        sxz, syz = s(w, SXZ, e), s(w, SYZ, e)
        if 0 in parts_of or 1 in parts_of:
            sxx, syy, sxy = s(w, SXX, e), s(w, SYY, e), s(w, SXY, e)
        forces = {}
        if 0 in parts_of:
            forces[0] = (s(w, SXX, e, after) - sxx) + b_y(sxy) + (sxz - s(w, SXZ, e - 1))
        if 1 in parts_of:
            forces[1] = (sxy - s(w, SXY, e, before)) + f_y(syy) + (syz - s(w, SYZ, e - 1))
        if 2 in parts_of:
            up = s(w, SZZ, e + 1) - s(w, SZZ, e)
            forces[2] = (sxz - s(w, SXZ, e, before)) + b_y(syz) + up
        buoyancy = m(0, e)
        for c, force in forces.items():
            moved = v(old, slot, w, c, e) + buoyancy * force
            if c == 2 and w == 1:
                moved = moved + inject[n, e + 1]
            if 0 <= e < depth:
                vel[1 - old, w, c, e, body, :] = moved
            else:
                vel_near[0 if e < 0 else 1, w, c, body, :] = moved

    def normal(parity, slot, w, e, n, spun=None, z_only=False):
        vx, vy, vz = [v(parity, slot, w, c, e) for c in range(3)]
        ex = vx - v(parity, slot, w, 0, e, before)
        ey = b_y(vy)
        ez = vz - v(parity, slot, w, 2, e - 1)
        common = m(1, e) * (ex + ey + ez)
        twice = 2.0 * m(2, e)
        if w == 0:
            common = common + source_at[e + 1] * wavelet[0, n]
        szz = add_s(w, SZZ, e, common + twice * ez)
        if z_only:
            return
        sxx = add_s(w, SXX, e, common + twice * ex)
        syy = add_s(w, SYY, e, common + twice * ey)
        if not 0 <= e < depth:
            return
        pressure = (sxx + syy + szz) * (1.0 / 3.0)
        if w == 0:
            press[parity, e] = pressure
        else:
            image[0, e] = image[0, e] + press[parity, e] * pressure
            if spun is not None:
                image[1, e] = image[1, e] + press[parity, e] * spin[spun]

    def shear(parity, slot, w, e, spun=None):
        vx, vy, vz = [v(parity, slot, w, c, e) for c in range(3)]
        x_up = v(parity, slot, w, 0, e + 1) - vx
        y_up = v(parity, slot, w, 1, e + 1) - vy
        z_along_x = v(parity, slot, w, 2, e, after) - vz
        z_along_y = f_y(vz)
        x_along_y = f_y(vx)
        y_along_x = v(parity, slot, w, 1, e, after) - vy
        mu = m(2, e)
        add_s(w, SXY, e, mu * (x_along_y + y_along_x))
        add_s(w, SXZ, e, mu * (x_up + z_along_x))
        add_s(w, SYZ, e, mu * (y_up + z_along_y))
        if w == 1:
            rotation = (z_along_y - y_up) + (x_up - z_along_x) + (y_along_x - x_along_y)
            if spun is None:
                image[1, e] = image[1, e] + press[parity, e] * rotation
            else:
                spin[spun] = rotation

    def shear_flat(parity, slot, w, e):
        x_along_y = f_y(v(parity, slot, w, 0, e))
        y_along_x = v(parity, slot, w, 1, e, after) - v(parity, slot, w, 1, e)
        add_s(w, SXY, e, m(2, e) * (x_along_y + y_along_x))

    def shear_deep(parity, slot, w, e):
        vx, vy, vz = [v(parity, slot, w, c, e) for c in range(3)]
        mu = m(2, e)
        z_along_x = v(parity, slot, w, 2, e, after) - vz
        add_s(w, SXZ, e, mu * ((v(parity, slot, w, 0, e + 1) - vx) + z_along_x))
        add_s(w, SYZ, e, mu * ((v(parity, slot, w, 1, e + 1) - vy) + f_y(vz)))

    def send_middle(cycle):
        for w in range(2):
            for side in range(2):
                up_to(goes[side], middle(w, cycle, side).start)

    def inside(cycle, n, send):
        for w in range(2):
            for e in range(1, depth):
                normal(0, None, w, e, n)
            shear(0, None, w, 0, spun=0)
            for e in range(1, last):
                shear(0, None, w, e)
            for e in (1, 2):
                velocity(w, e, n + 1, 0, None)
            normal(1, None, w, 2, n + 1)
            shear(1, None, w, 1, spun=1)
        up_to(send, lambda: send_middle(cycle))

    def lower(slot, w, n, final):
        up_to(goes[0], message(w, slot, 0).wait_send)
        up_to(comes[1], message(w, slot, 1).wait_recv)
        shear(0, slot, w, last)
        normal(0, slot, w, depth, n)
        shear_flat(0, slot, w, depth)
        shear_deep(0, slot, w, depth)
        if not final:
            normal(0, slot, w, depth + 1, n, z_only=True)
        velocity(w, last, n + 1, 0, slot)
        velocity(w, depth, n + 1, 0, slot, (0, 1) if final else (0, 1, 2))
        normal(1, slot, w, last, n + 1)
        shear(1, slot, w, last - 1)
        shear(1, slot, w, last)
        if final:
            return
        normal(1, slot, w, depth, n + 1)
        velocity(w, last, n + 2, 1, slot)
        velocity(w, last - 1, n + 2, 1, slot)
        up_to(goes[0], message(w, 1 - slot, 0).start)
        shear_flat(1, slot, w, depth)

    def upper(slot, w, n, final):
        up_to(comes[0], message(w, slot, 0).wait_recv)
        normal(0, slot, w, 0, n, spun=0)
        shear_deep(0, slot, w, -1)
        normal(0, slot, w, -1, n, z_only=final)
        if not final:
            shear_flat(0, slot, w, -1)
            shear_deep(0, slot, w, -2)
        velocity(w, 0, n + 1, 0, slot)
        velocity(w, -1, n + 1, 0, slot, (2,) if final else (0, 1, 2))
        normal(1, slot, w, 0, n + 1)
        normal(1, slot, w, 1, n + 1, spun=1)
        shear(1, slot, w, 0)
        up_to(goes[1], message(w, slot, 1).wait_send)
        if final:
            return
        shear_deep(1, slot, w, -1)
        velocity(w, 0, n + 2, 1, slot)
        velocity(w, 1, n + 2, 1, slot)
        up_to(goes[1], message(w, 1 - slot, 1).start)
        shear_flat(1, slot, w, -1)

    def catch_up(cycle, n):
        for w in range(2):
            for side in range(2):
                up_to(comes[side], middle(w, cycle, side).wait_recv)
        for w in range(2):
            shear_deep(1, cycle, w, depth)
            normal(1, cycle, w, depth + 1, n, z_only=True)
            normal(1, cycle, w, -1, n)
            shear_deep(1, cycle, w, -2)

    up_to(comes[1], first_up[0].wait_recv)
    for w in range(2):
        velocity(w, last, 0, 1, None)
        velocity(w, last - 1, 0, 1, None)
        up_to(goes[0], message(w, 0, 0).start)
    for w in range(2):
        velocity(w, 1, 0, 1, None)
        velocity(w, 0, 0, 1, None, (2,))
        for e in range(1, depth):
            normal(0, None, w, e, 0)
        for e in range(1, last):
            shear(0, None, w, e)
        velocity(w, 2, 1, 0, None)
        velocity(w, 1, 1, 0, None, (2,))
        normal(1, None, w, 2, 1)

    def upper_side_is_there():
        pl.semaphore_wait(near_sem.at[0], 1)
        for copy in first_up:
            copy.start()
        for hop in others:
            to = {"shot": lax.rem(shot + hop, shots)}
            pl.semaphore_signal(peers_sem, inc=1, device_id=to, device_id_type=MESH)

    up_to(odd, upper_side_is_there)
    up_to(comes[0], first_down[0].wait_recv)
    for w in range(2):
        velocity(w, 0, 0, 1, None, (0, 1))
    for w in range(2):
        up_to(goes[1], message(w, 0, 1).start)
    for w in range(2):
        shear(0, None, w, 0, spun=0)
        velocity(w, 1, 1, 0, None, (0, 1))
        shear(1, None, w, 1, spun=1)
    send_middle(0)
    up_to(comes[1], lambda: [copy.wait_recv() for copy in first_up[1:]])
    up_to(comes[0], lambda: [copy.wait_recv() for copy in first_down[1:]])
    mat_near[...] = time_step * mat_near[...]
    mat_far[...] = time_step * mat_far[...]

    up_to(has_down, first_down[0].wait_send)
    up_to(has_up, first_up[0].wait_send)

    cycles = steps // 2

    def cycle_body(cycle, carry):
        slot = lax.rem(cycle, 2)
        n = 2 * cycle
        for w in range(2):
            lower(slot, w, n, False)
        for w in range(2):
            upper(slot, w, n, False)
        for w in range(2):
            for side in range(2):
                up_to(goes[side], middle(w, cycle, side).wait_send)
        inside(cycle + 1, n + 2, cycle < cycles - 2)
        catch_up(cycle, n + 1)
        return carry

    lax.fori_loop(0, cycles - 1, cycle_body, 0)

    def to_shot(half, hop, source):
        planes = pl.ds(2 * half, 2)
        return remote(
            image.at[:, planes],
            out.at[source, :, planes],
            sum_send.at[half, hop],
            sum_recv.at[half, hop],
            shot=lax.rem(shot + hop, shots),
        )

    def keep(half):
        planes = pl.ds(2 * half, 2)
        return pltpu.make_async_copy(image.at[:, planes], out.at[shot, :, planes], keep_sem.at[half])

    def hand_over(half):
        for hop in (2, 1, 3):
            to_shot(half, hop, shot).start()
        keep(half).start()

    def pass_on():
        pl.semaphore_wait(peers_sem, shots - 1)
        pl.semaphore_signal(ready_sem, inc=1, device_id={"gz": here - 1}, device_id_type=MESH)

    up_to(odd, pass_on)
    end = (cycles - 1) % 2
    for w in range(2):
        upper(end, w, steps - 2, True)
    up_to(even, lambda: pl.semaphore_wait(ready_sem, 1))
    hand_over(0)
    for w in range(2):
        lower(end, w, steps - 2, True)
    hand_over(1)
    up_to(has_down, lambda: [copy.wait_send() for copy in first_down[1:]])
    up_to(has_up, lambda: [copy.wait_send() for copy in first_up[1:]])
    for half in (1, 0):
        keep(half).wait()
        for hop in others:
            to_shot(half, hop, lax.rem(shot + shots - hop, shots)).wait_recv()
    for half in (1, 0):
        for hop in others:
            to_shot(half, hop, shot).wait_send()


def solution(mesh):
    slabs, shots = mesh.shape["gz"], mesh.shape["shot"]

    def on_device(wavefields, earth, s_depth, s_column, wavelet, r_depth, r_column, traces):
        depth, rows, cols = earth.shape[1:]
        steps, receivers = traces.shape[1:]
        assert depth == 4 and shots == 4 and slabs % 2 == 0 and steps % 2 == 0 and steps >= 4
        dims = (slabs, shots, depth, rows, cols, steps, receivers)
        padded = rows + 2 * GUARD
        f32 = jnp.float32
        mids = steps // 2 - 1
        hbm = pl.BlockSpec(memory_space=pltpu.HBM)
        dma = pltpu.SemaphoreType.DMA
        by_shot = pl.pallas_call(
            functools.partial(window_kernel, dims),
            out_shape=jax.ShapeDtypeStruct((shots, 2, depth, rows, cols), f32),
            in_specs=[hbm] * 8,
            out_specs=hbm,
            scratch_shapes=[
                pltpu.VMEM((2, 2, 3, depth, padded, cols), f32),
                pltpu.VMEM((2, 2, 2, 3, 2, padded, cols), f32),
                pltpu.VMEM((mids, 2, 2, 3, padded, cols), f32),
                pltpu.VMEM((2, 2, 3, padded, cols), f32),
                pltpu.VMEM((2, 6, depth, padded, cols), f32),
                pltpu.VMEM((2, 2, 6, padded, cols), f32),
                pltpu.VMEM((2, 3, rows, cols), f32),
                pltpu.VMEM((3, depth, rows, cols), f32),
                pltpu.VMEM((2, 3, rows, cols), f32),
                pltpu.VMEM((3, rows, cols), f32),
                pltpu.VMEM((depth + 3, rows, cols), f32),
                pltpu.VMEM((steps, depth + 2, rows, cols), f32),
                pltpu.VMEM((2, depth, rows, cols), f32),
                pltpu.VMEM((2, rows, cols), f32),
                pltpu.VMEM((2, depth, rows, cols), f32),
                pltpu.VMEM((2, steps, 2 * receivers), f32),
                pltpu.SMEM(s_depth.shape, jnp.int32),
                pltpu.SMEM(s_column.shape, jnp.int32),
                pltpu.SMEM(wavelet.shape, f32),
                pltpu.VMEM(r_depth.shape, jnp.int32),
                pltpu.VMEM(r_column.shape, jnp.int32),
                pltpu.VMEM(traces.shape, f32),
                dma((3,)),
                dma((6,)),
                dma((2,)),
                pltpu.SemaphoreType.REGULAR((2,)),
                pltpu.SemaphoreType.REGULAR,
                pltpu.SemaphoreType.REGULAR,
                dma((2, 6)),
                dma((2, 6)),
                dma((2, 2, 2)),
                dma((2, 2, 2)),
                dma((mids, 2, 2)),
                dma((mids, 2, 2)),
                dma((2, shots)),
                dma((2, shots)),
            ],
            compiler_params=pltpu.CompilerParams(
                collective_id=0, has_side_effects=True
            ),
        )(wavefields[0], earth, s_depth, s_column, wavelet, r_depth, r_column, traces)
        return sum(by_shot[i] for i in range(1, shots)) / steps + by_shot[0] / steps

    sharded = P(("parts", "shot"))
    return jax.shard_map(
        on_device,
        mesh=mesh,
        in_specs=(
            P(("parts", "shot"), None, None, "gz", None, None),
            P("parts", "gz", None, None),
            sharded,
            sharded,
            P(("parts", "shot"), None),
            P(("parts", "shot"), None),
            P(("parts", "shot"), None),
            P(("parts", "shot"), None, None),
        ),
        out_specs=P("parts", "gz", None, None),
        check_vma=False,
    )
```

```python
import functools
import itertools

import jax
import jax.numpy as jnp
from jax import lax
from jax.experimental import pallas as pl
from jax.experimental.pallas import tpu as pltpu
from jax.sharding import PartitionSpec as P

MESH = pl.DeviceIdType.MESH
time_step = 0.15
GUARD = 8
SXX, SYY, SZZ, SXY, SXZ, SYZ = range(6)


def window_kernel(
    dims,
    fields_in,
    earth_in,
    source_depth_in,
    source_column_in,
    wavelet_in,
    receiver_depth_in,
    receiver_column_in,
    traces_in,
    out,
    vel,
    vel_msg,
    vel_mid,
    vel_near,
    sig,
    sig_near,
    sig_far,
    mat,
    mat_near,
    mat_far,
    source_at,
    inject,
    press,
    spin,
    image,
    parts,
    source_depth,
    source_column,
    wavelet,
    receiver_depth,
    receiver_column,
    traces,
    load_sem,
    small_sem,
    keep_sem,
    near_sem,
    peers_sem,
    ready_sem,
    first_send,
    first_recv,
    msg_send,
    msg_recv,
    mid_send,
    mid_recv,
    sum_send,
    sum_recv,
):
    slabs, shots, depth, rows, cols, steps, receivers = dims
    here = lax.axis_index("gz")
    shot = lax.axis_index("shot")
    has_up, has_down = here > 0, here < slabs - 1
    last = depth - 1
    whole = pl.ds(0, rows)
    body = pl.ds(GUARD, rows)
    after = pl.ds(GUARD + 1, rows)
    before = pl.ds(GUARD - 1, rows)
    lane = lax.broadcasted_iota(jnp.int32, (rows, cols), 1)
    row = lax.broadcasted_iota(jnp.int32, (rows, cols), 0)
    at_first, at_last = lane == 0, lane == cols - 1

    def b_y(f):
        return f - jnp.where(at_first, 0.0, pltpu.roll(f, 1, 1))

    def f_y(f):
        return jnp.where(at_last, 0.0, pltpu.roll(f, cols - 1, 1)) - f

    loads = [
        pltpu.make_async_copy(src, dst, load_sem.at[i])
        for i, (src, dst) in enumerate(
            (
                (fields_in.at[:, 7:9], sig.at[:, 4:6, :, body, :]),
                (fields_in.at[:, 5:6], sig.at[:, 2:3, :, body, :]),
                (fields_in.at[:, 3:5], sig.at[:, 0:2, :, body, :]),
                (fields_in.at[:, 6:7], sig.at[:, 3:4, :, body, :]),
                (fields_in.at[:, 0:3], vel.at[1, :, :, :, body, :]),
                (earth_in, mat),
            )
        )
    ]
    small = [
        pltpu.make_async_copy(src, dst, small_sem.at[i])
        for i, (src, dst) in enumerate(
            (
                (source_depth_in, source_depth),
                (source_column_in, source_column),
                (wavelet_in, wavelet),
                (receiver_depth_in, receiver_depth),
                (receiver_column_in, receiver_column),
                (traces_in, traces),
            )
        )
    ]
    for copy in loads + small:
        copy.start()

    barrier = pltpu.get_barrier_semaphore()

    def up_to(where, then):
        @pl.when(where)
        def _():
            then()

    def greet(**to):
        pl.semaphore_signal(barrier, inc=1, device_id=to, device_id_type=MESH)

    others = range(1, shots)
    odd = lax.rem(here, 2) == 1
    even = lax.rem(here, 2) == 0

    def greet_all():
        greet(gz=here - 1)
        up_to(has_down, lambda: greet(gz=here + 1))
        for hop in others:
            greet(shot=lax.rem(shot + hop, shots))

    def answer(side, **to):
        pl.semaphore_signal(near_sem.at[side], inc=1, device_id=to, device_id_type=MESH)

    up_to(odd, greet_all)
    beside = jnp.where(has_up, 1, 0) + jnp.where(has_down, 1, 0)
    pl.semaphore_wait(barrier, jnp.where(even, beside, shots - 1))
    up_to(even & has_down, lambda: answer(0, gz=here + 1))
    up_to(even & has_up, lambda: answer(1, gz=here - 1))

    def remote(src, dst, send, recv, **to):
        return pltpu.make_async_remote_copy(
            src_ref=src, dst_ref=dst, send_sem=send, recv_sem=recv, device_id=to, device_id_type=MESH
        )

    downs = (
        (sig.at[:, 4:6, last, body, :], sig_near.at[0, :, 4:6, body, :]),
        (fields_in.at[:, 3:7, last], sig_near.at[0, :, 0:4, body, :]),
        (fields_in.at[:, 7:9, last - 1], sig_far.at[:, 0:2]),
        (earth_in.at[:, last], mat_near.at[0]),
        (earth_in.at[2, last - 1], mat_far.at[0]),
    )
    ups = (
        (sig.at[:, 2:3, 0, body, :], sig_near.at[1, :, 2:3, body, :]),
        (fields_in.at[:, 3:5, 0], sig_near.at[1, :, 0:2, body, :]),
        (fields_in.at[:, 6:9, 0], sig_near.at[1, :, 3:6, body, :]),
        (fields_in.at[:, 5, 1], sig_far.at[:, 2]),
        (earth_in.at[:, 0], mat_near.at[1]),
        (earth_in.at[1:3, 1], mat_far.at[1:3]),
    )
    first_down = [
        remote(src, dst, first_send.at[0, i], first_recv.at[0, i], gz=here + 1)
        for i, (src, dst) in enumerate(downs)
    ]
    first_up = [
        remote(src, dst, first_send.at[1, i], first_recv.at[1, i], gz=here - 1)
        for i, (src, dst) in enumerate(ups)
    ]
    loads[0].wait()
    loads[1].wait()
    up_to(odd & has_down, lambda: pl.semaphore_wait(near_sem.at[1], 1))
    up_to(has_down, first_down[0].start)
    up_to(even & has_up, first_up[0].start)
    up_to(has_down, lambda: [copy.start() for copy in first_down[1:]])
    up_to(even & has_up, lambda: [copy.start() for copy in first_up[1:]])

    zeros = jnp.zeros((GUARD, cols), jnp.float32)

    def clear_around(ref, *extents):
        for index in itertools.product(*[range(extent) for extent in extents]):
            ref[(*index, pl.ds(0, GUARD), slice(None))] = zeros
            ref[(*index, pl.ds(GUARD + rows, GUARD), slice(None))] = zeros

    clear_around(sig, 2, 6, depth)
    clear_around(vel, 2, 2, 3, depth)
    clear_around(vel_near, 2, 2, 3)
    clear_around(vel_msg, 2, 2, 2, 3, 2)
    clear_around(vel_mid, steps // 2 - 1, 2, 2, 3)
    clear_around(sig_near, 2, 2, 6)

    def outside(side):
        far = pl.ds(0, 2) if side == 0 else pl.ds(2, 1)
        for view in (
            vel_msg.at[:, side, :, :, :, body, :],
            vel_mid.at[:, side, :, :, body, :],
            sig_near.at[side, :, :, body, :],
            sig_far.at[:, far],
            mat_near.at[side],
            mat_far.at[pl.ds(side, 1 + side)],
        ):
            view[...] = jnp.zeros(view.shape, jnp.float32)

    up_to(here == 0, lambda: outside(0))
    up_to(here == slabs - 1, lambda: outside(1))

    def message(w, slot, side):
        planes = pl.ds(depth - 2, 2) if side == 0 else pl.ds(0, 2)
        return remote(
            vel.at[0, w, :, planes, body, :],
            vel_msg.at[slot, side, w, :, :, body, :],
            msg_send.at[slot, side, w],
            msg_recv.at[slot, side, w],
            gz=here + 1 if side == 0 else here - 1,
        )

    def middle(w, cycle, side):
        return remote(
            vel.at[1, w, :, depth - 2 if side == 0 else 1, body, :],
            vel_mid.at[cycle, side, w, :, body, :],
            mid_send.at[cycle, side, w],
            mid_recv.at[cycle, side, w],
            gz=here + 1 if side == 0 else here - 1,
        )

    goes = (has_down, has_up)
    comes = (has_up, has_down)

    for copy in small:
        copy.wait()
    source_row = (source_depth[0] - here * depth + 1) * rows + source_column[0] // cols
    source_col = source_column[0] % cols
    for z in range(depth + 3):
        hit = (row + z * rows == source_row) & (lane == source_col)
        source_at[z] = jnp.where(hit, time_step, 0.0)
    cells = (depth + 2) * rows
    receiver_row = (receiver_depth[...] - here * depth + 1) * rows + receiver_column[...] // cols
    receiver_col = receiver_column[...] % cols
    twice_row = jnp.concatenate([receiver_row, receiver_row], axis=1)
    twice_col = jnp.concatenate([receiver_col, receiver_col], axis=1)
    in_row = lax.broadcasted_iota(jnp.int32, (cells, 2 * receivers), 0) == twice_row
    in_col = lax.broadcasted_iota(jnp.int32, (cols, 2 * receivers), 0) == twice_col
    in_col = jnp.where(in_col, 1.0, 0.0).astype(jnp.bfloat16)
    in_col = jnp.concatenate([in_col, in_col], axis=1)

    def in_bf16(f):
        return f.astype(jnp.bfloat16).astype(jnp.float32)

    amounts = time_step * traces[0]
    high = in_bf16(amounts)
    middle_part = in_bf16(amounts - high)
    low = in_bf16((amounts - high) - middle_part)
    parts[0] = jnp.concatenate([high, middle_part], axis=1)
    parts[1] = jnp.concatenate([low, jnp.zeros_like(low)], axis=1)

    def receivers_at(n, carry):
        spread = [
            jnp.where(in_row, parts[i, pl.ds(n, 1), :], 0.0).astype(jnp.bfloat16) for i in range(2)
        ]
        inject[n] = lax.dot_general(
            jnp.concatenate(spread, axis=1),
            in_col,
            (((1,), (1,)), ((), ())),
            preferred_element_type=jnp.float32,
        ).reshape(depth + 2, rows, cols)
        return carry

    lax.fori_loop(0, steps, receivers_at, 0)
    image[...] = jnp.zeros_like(image)

    for copy in loads[2:]:
        copy.wait()
    mat[...] = time_step * mat[...]

    def v(parity, slot, w, c, e, at=body):
        if 0 <= e < depth:
            return vel[parity, w, c, e, at, :]
        side = 0 if e < 0 else 1
        if parity == 0:
            return vel_msg[slot, side, w, c, e + 2 if e < 0 else e - depth, at, :]
        if e in (-1, depth):
            return vel_near[side, w, c, at, :]
        return vel_mid[slot, side, w, c, at, :]

    def s_at(w, f, e):
        if 0 <= e < depth:
            return sig, (w, f, e), True
        if e in (-1, depth):
            return sig_near, (0 if e < 0 else 1, w, f), True
        return sig_far, (w, {SXZ: 0, SYZ: 1, SZZ: 2}[f]), False

    def s(w, f, e, at=body):
        ref, index, guarded = s_at(w, f, e)
        return ref[(*index, at if guarded else whole, slice(None))]

    def add_s(w, f, e, change):
        ref, index, guarded = s_at(w, f, e)
        value = ref[(*index, body if guarded else whole, slice(None))] + change
        ref[(*index, body if guarded else whole, slice(None))] = value
        return value

    def m(which, e):
        if 0 <= e < depth:
            return mat[which, e]
        if e in (-1, depth):
            return mat_near[0 if e < 0 else 1, which]
        return mat_far[0 if e < 0 else which]

    def velocity(w, e, n, old, slot, parts_of=(0, 1, 2)):
        sxz, syz = s(w, SXZ, e), s(w, SYZ, e)
        if 0 in parts_of or 1 in parts_of:
            sxx, syy, sxy = s(w, SXX, e), s(w, SYY, e), s(w, SXY, e)
        forces = {}
        if 0 in parts_of:
            forces[0] = (s(w, SXX, e, after) - sxx) + b_y(sxy) + (sxz - s(w, SXZ, e - 1))
        if 1 in parts_of:
            forces[1] = (sxy - s(w, SXY, e, before)) + f_y(syy) + (syz - s(w, SYZ, e - 1))
        if 2 in parts_of:
            up = s(w, SZZ, e + 1) - s(w, SZZ, e)
            forces[2] = (sxz - s(w, SXZ, e, before)) + b_y(syz) + up
        buoyancy = m(0, e)
        for c, force in forces.items():
            moved = v(old, slot, w, c, e) + buoyancy * force
            if c == 2 and w == 1:
                moved = moved + inject[n, e + 1]
            if 0 <= e < depth:
                vel[1 - old, w, c, e, body, :] = moved
            else:
                vel_near[0 if e < 0 else 1, w, c, body, :] = moved

    def normal(parity, slot, w, e, n, spun=None, z_only=False):
        vx, vy, vz = [v(parity, slot, w, c, e) for c in range(3)]
        ex = vx - v(parity, slot, w, 0, e, before)
        ey = b_y(vy)
        ez = vz - v(parity, slot, w, 2, e - 1)
        common = m(1, e) * (ex + ey + ez)
        twice = 2.0 * m(2, e)
        if w == 0:
            common = common + source_at[e + 1] * wavelet[0, n]
        szz = add_s(w, SZZ, e, common + twice * ez)
        if z_only:
            return
        sxx = add_s(w, SXX, e, common + twice * ex)
        syy = add_s(w, SYY, e, common + twice * ey)
        if not 0 <= e < depth:
            return
        pressure = (sxx + syy + szz) * (1.0 / 3.0)
        if w == 0:
            press[parity, e] = pressure
        else:
            image[0, e] = image[0, e] + press[parity, e] * pressure
            if spun is not None:
                image[1, e] = image[1, e] + press[parity, e] * spin[spun]

    def shear(parity, slot, w, e, spun=None):
        vx, vy, vz = [v(parity, slot, w, c, e) for c in range(3)]
        x_up = v(parity, slot, w, 0, e + 1) - vx
        y_up = v(parity, slot, w, 1, e + 1) - vy
        z_along_x = v(parity, slot, w, 2, e, after) - vz
        z_along_y = f_y(vz)
        x_along_y = f_y(vx)
        y_along_x = v(parity, slot, w, 1, e, after) - vy
        mu = m(2, e)
        add_s(w, SXY, e, mu * (x_along_y + y_along_x))
        add_s(w, SXZ, e, mu * (x_up + z_along_x))
        add_s(w, SYZ, e, mu * (y_up + z_along_y))
        if w == 1:
            rotation = (z_along_y - y_up) + (x_up - z_along_x) + (y_along_x - x_along_y)
            if spun is None:
                image[1, e] = image[1, e] + press[parity, e] * rotation
            else:
                spin[spun] = rotation

    def shear_flat(parity, slot, w, e):
        x_along_y = f_y(v(parity, slot, w, 0, e))
        y_along_x = v(parity, slot, w, 1, e, after) - v(parity, slot, w, 1, e)
        add_s(w, SXY, e, m(2, e) * (x_along_y + y_along_x))

    def shear_deep(parity, slot, w, e):
        vx, vy, vz = [v(parity, slot, w, c, e) for c in range(3)]
        mu = m(2, e)
        z_along_x = v(parity, slot, w, 2, e, after) - vz
        add_s(w, SXZ, e, mu * ((v(parity, slot, w, 0, e + 1) - vx) + z_along_x))
        add_s(w, SYZ, e, mu * ((v(parity, slot, w, 1, e + 1) - vy) + f_y(vz)))

    def send_middle(cycle):
        for w in range(2):
            for side in range(2):
                up_to(goes[side], middle(w, cycle, side).start)

    def inside(cycle, n, send):
        for w in range(2):
            for e in range(1, depth):
                normal(0, None, w, e, n)
            shear(0, None, w, 0, spun=0)
            for e in range(1, last):
                shear(0, None, w, e)
            for e in (1, 2):
                velocity(w, e, n + 1, 0, None)
            normal(1, None, w, 2, n + 1)
            shear(1, None, w, 1, spun=1)
        up_to(send, lambda: send_middle(cycle))

    def lower(slot, w, n, final):
        up_to(goes[0], message(w, slot, 0).wait_send)
        up_to(comes[1], message(w, slot, 1).wait_recv)
        shear(0, slot, w, last)
        normal(0, slot, w, depth, n)
        shear_flat(0, slot, w, depth)
        shear_deep(0, slot, w, depth)
        if not final:
            normal(0, slot, w, depth + 1, n, z_only=True)
        velocity(w, last, n + 1, 0, slot)
        velocity(w, depth, n + 1, 0, slot, (0, 1) if final else (0, 1, 2))
        normal(1, slot, w, last, n + 1)
        shear(1, slot, w, last - 1)
        shear(1, slot, w, last)
        if final:
            return
        normal(1, slot, w, depth, n + 1)
        velocity(w, last, n + 2, 1, slot)
        velocity(w, last - 1, n + 2, 1, slot)
        up_to(goes[0], message(w, 1 - slot, 0).start)
        shear_flat(1, slot, w, depth)

    def upper(slot, w, n, final):
        up_to(comes[0], message(w, slot, 0).wait_recv)
        normal(0, slot, w, 0, n, spun=0)
        shear_deep(0, slot, w, -1)
        normal(0, slot, w, -1, n, z_only=final)
        if not final:
            shear_flat(0, slot, w, -1)
            shear_deep(0, slot, w, -2)
        velocity(w, 0, n + 1, 0, slot)
        velocity(w, -1, n + 1, 0, slot, (2,) if final else (0, 1, 2))
        normal(1, slot, w, 0, n + 1)
        normal(1, slot, w, 1, n + 1, spun=1)
        shear(1, slot, w, 0)
        up_to(goes[1], message(w, slot, 1).wait_send)
        if final:
            return
        shear_deep(1, slot, w, -1)
        velocity(w, 0, n + 2, 1, slot)
        velocity(w, 1, n + 2, 1, slot)
        up_to(goes[1], message(w, 1 - slot, 1).start)
        shear_flat(1, slot, w, -1)

    def catch_up(cycle, n):
        for w in range(2):
            for side in range(2):
                up_to(comes[side], middle(w, cycle, side).wait_recv)
        for w in range(2):
            shear_deep(1, cycle, w, depth)
            normal(1, cycle, w, depth + 1, n, z_only=True)
            normal(1, cycle, w, -1, n)
            shear_deep(1, cycle, w, -2)

    up_to(comes[1], first_up[0].wait_recv)
    for w in range(2):
        velocity(w, last, 0, 1, None)
        velocity(w, last - 1, 0, 1, None)
        up_to(goes[0], message(w, 0, 0).start)
    for w in range(2):
        velocity(w, 1, 0, 1, None)
        velocity(w, 0, 0, 1, None, (2,))
        for e in range(1, depth):
            normal(0, None, w, e, 0)
        for e in range(1, last):
            shear(0, None, w, e)
        velocity(w, 2, 1, 0, None)
        velocity(w, 1, 1, 0, None, (2,))
        normal(1, None, w, 2, 1)

    def upper_side_is_there():
        pl.semaphore_wait(near_sem.at[0], 1)
        for copy in first_up:
            copy.start()
        for hop in others:
            to = {"shot": lax.rem(shot + hop, shots)}
            pl.semaphore_signal(peers_sem, inc=1, device_id=to, device_id_type=MESH)

    up_to(odd, upper_side_is_there)
    up_to(comes[0], first_down[0].wait_recv)
    for w in range(2):
        velocity(w, 0, 0, 1, None, (0, 1))
    for w in range(2):
        up_to(goes[1], message(w, 0, 1).start)
    for w in range(2):
        shear(0, None, w, 0, spun=0)
        velocity(w, 1, 1, 0, None, (0, 1))
        shear(1, None, w, 1, spun=1)
    send_middle(0)
    up_to(comes[1], lambda: [copy.wait_recv() for copy in first_up[1:]])
    up_to(comes[0], lambda: [copy.wait_recv() for copy in first_down[1:]])
    mat_near[...] = time_step * mat_near[...]
    mat_far[...] = time_step * mat_far[...]

    up_to(has_down, first_down[0].wait_send)
    up_to(has_up, first_up[0].wait_send)

    cycles = steps // 2

    def cycle_body(cycle, carry):
        slot = lax.rem(cycle, 2)
        n = 2 * cycle
        for w in range(2):
            lower(slot, w, n, False)
        for w in range(2):
            upper(slot, w, n, False)
        for w in range(2):
            for side in range(2):
                up_to(goes[side], middle(w, cycle, side).wait_send)
        inside(cycle + 1, n + 2, cycle < cycles - 2)
        catch_up(cycle, n + 1)
        return carry

    lax.fori_loop(0, cycles - 1, cycle_body, 0)

    def to_shot(half, hop, source):
        planes = pl.ds(2 * half, 2)
        return remote(
            image.at[:, planes],
            out.at[source, :, planes],
            sum_send.at[half, hop],
            sum_recv.at[half, hop],
            shot=lax.rem(shot + hop, shots),
        )

    def keep(half):
        planes = pl.ds(2 * half, 2)
        return pltpu.make_async_copy(image.at[:, planes], out.at[shot, :, planes], keep_sem.at[half])

    def hand_over(half):
        for hop in (1, 2, 3):
            to_shot(half, hop, shot).start()
        keep(half).start()

    def pass_on():
        pl.semaphore_wait(peers_sem, shots - 1)
        pl.semaphore_signal(ready_sem, inc=1, device_id={"gz": here - 1}, device_id_type=MESH)

    up_to(odd, pass_on)
    end = (cycles - 1) % 2
    for w in range(2):
        upper(end, w, steps - 2, True)
    up_to(even, lambda: pl.semaphore_wait(ready_sem, 1))
    hand_over(0)
    for w in range(2):
        lower(end, w, steps - 2, True)
    hand_over(1)
    up_to(has_down, lambda: [copy.wait_send() for copy in first_down[1:]])
    up_to(has_up, lambda: [copy.wait_send() for copy in first_up[1:]])
    for half in (1, 0):
        keep(half).wait()
        for hop in others:
            to_shot(half, hop, lax.rem(shot + shots - hop, shots)).wait_recv()
    for half in (1, 0):
        for hop in others:
            to_shot(half, hop, shot).wait_send()


def solution(mesh):
    slabs, shots = mesh.shape["gz"], mesh.shape["shot"]

    def on_device(wavefields, earth, s_depth, s_column, wavelet, r_depth, r_column, traces):
        depth, rows, cols = earth.shape[1:]
        steps, receivers = traces.shape[1:]
        assert depth == 4 and shots == 4 and slabs % 2 == 0 and steps % 2 == 0 and steps >= 4
        dims = (slabs, shots, depth, rows, cols, steps, receivers)
        padded = rows + 2 * GUARD
        f32 = jnp.float32
        mids = steps // 2 - 1
        hbm = pl.BlockSpec(memory_space=pltpu.HBM)
        dma = pltpu.SemaphoreType.DMA
        by_shot = pl.pallas_call(
            functools.partial(window_kernel, dims),
            out_shape=jax.ShapeDtypeStruct((shots, 2, depth, rows, cols), f32),
            in_specs=[hbm] * 8,
            out_specs=hbm,
            scratch_shapes=[
                pltpu.VMEM((2, 2, 3, depth, padded, cols), f32),
                pltpu.VMEM((2, 2, 2, 3, 2, padded, cols), f32),
                pltpu.VMEM((mids, 2, 2, 3, padded, cols), f32),
                pltpu.VMEM((2, 2, 3, padded, cols), f32),
                pltpu.VMEM((2, 6, depth, padded, cols), f32),
                pltpu.VMEM((2, 2, 6, padded, cols), f32),
                pltpu.VMEM((2, 3, rows, cols), f32),
                pltpu.VMEM((3, depth, rows, cols), f32),
                pltpu.VMEM((2, 3, rows, cols), f32),
                pltpu.VMEM((3, rows, cols), f32),
                pltpu.VMEM((depth + 3, rows, cols), f32),
                pltpu.VMEM((steps, depth + 2, rows, cols), f32),
                pltpu.VMEM((2, depth, rows, cols), f32),
                pltpu.VMEM((2, rows, cols), f32),
                pltpu.VMEM((2, depth, rows, cols), f32),
                pltpu.VMEM((2, steps, 2 * receivers), f32),
                pltpu.SMEM(s_depth.shape, jnp.int32),
                pltpu.SMEM(s_column.shape, jnp.int32),
                pltpu.SMEM(wavelet.shape, f32),
                pltpu.VMEM(r_depth.shape, jnp.int32),
                pltpu.VMEM(r_column.shape, jnp.int32),
                pltpu.VMEM(traces.shape, f32),
                dma((6,)),
                dma((6,)),
                dma((2,)),
                pltpu.SemaphoreType.REGULAR((2,)),
                pltpu.SemaphoreType.REGULAR,
                pltpu.SemaphoreType.REGULAR,
                dma((2, 6)),
                dma((2, 6)),
                dma((2, 2, 2)),
                dma((2, 2, 2)),
                dma((mids, 2, 2)),
                dma((mids, 2, 2)),
                dma((2, shots)),
                dma((2, shots)),
            ],
            compiler_params=pltpu.CompilerParams(
                collective_id=0, has_side_effects=True
            ),
        )(wavefields[0], earth, s_depth, s_column, wavelet, r_depth, r_column, traces)
        return sum(by_shot[i] for i in range(1, shots)) / steps + by_shot[0] / steps

    sharded = P(("parts", "shot"))
    return jax.shard_map(
        on_device,
        mesh=mesh,
        in_specs=(
            P(("parts", "shot"), None, None, "gz", None, None),
            P("parts", "gz", None, None),
            sharded,
            sharded,
            P(("parts", "shot"), None),
            P(("parts", "shot"), None),
            P(("parts", "shot"), None),
            P(("parts", "shot"), None, None),
        ),
        out_specs=P("parts", "gz", None, None),
        check_vma=False,
    )
```
